32 devices in a mesh: rep: 4 (over x, y), dp: 8 (over z, core).
Axes of the slice: x: 2, y: 2, z: 4, core: 2. Of those that a mesh axis runs over, the one named last changes fastest.
Arguments:
- x: bfloat16 [32, 2048, 1024], P(('rep', 'dp')), parts along dimension 0
- dy: bfloat16 [32, 2048, 1024], P(('rep', 'dp')), parts along dimension 0
- w_gate: bfloat16 [2, 1024, 4096], replicated
- w_up: bfloat16 [2, 1024, 4096], replicated
- w_down: bfloat16 [2, 4096, 1024], replicated
- m_w_gate: float32 [2, 1024, 4096], replicated
- m_w_up: float32 [2, 1024, 4096], replicated
- m_w_down: float32 [2, 4096, 1024], replicated
- v_w_gate: float32 [2, 1024, 4096], replicated
- v_w_up: float32 [2, 1024, 4096], replicated
- v_w_down: float32 [2, 4096, 1024], replicated
Outputs:
- output 1: bfloat16 [8, 1024, 4096], P('rep'), parts along dimension 0
- output 2: bfloat16 [8, 1024, 4096], P('rep'), parts along dimension 0
- output 3: bfloat16 [8, 4096, 1024], P('rep'), parts along dimension 0
- output 4: float32 [8, 1024, 4096], P('rep'), parts along dimension 0
- output 5: float32 [8, 1024, 4096], P('rep'), parts along dimension 0
- output 6: float32 [8, 4096, 1024], P('rep'), parts along dimension 0
- output 7: float32 [8, 1024, 4096], P('rep'), parts along dimension 0
- output 8: float32 [8, 1024, 4096], P('rep'), parts along dimension 0
- output 9: float32 [8, 4096, 1024], P('rep'), parts along dimension 0
There are 4 independent parts. The reference program is written for one: setup_inputs(seed, part) draws one part's arguments, and reference() takes and returns one part's arrays. A program takes and returns all parts, laid end to end along the dimension named above; an argument that names none is the same for every part.
All inputs are finite; a program needn't handle non-finite values.
Results may differ from the reference program's by a relative error of at most 0.022.
Values are sent between devices in bfloat16 or wider.
A program may use at most 2.75 GiB of HBM per device.

```python
import jax
import jax.numpy as jnp
from jax import lax

SEQUENCES = 8
TOKENS = 2048
D = 1024
FF = 4096
LAYERS = 2
NAMES = ("w_gate", "w_up", "w_down")
SHAPES = {"w_gate": (LAYERS, D, FF), "w_up": (LAYERS, D, FF), "w_down": (LAYERS, FF, D)}


def bump(key, n, height):
    away = (jnp.arange(n, dtype=jnp.int32) - jax.random.randint(key, (), 0, n, jnp.int32)) % n
    return jnp.where(away < n // 8, height, 1.0)


def together(key, own, strength):
    shared = jax.random.normal(key, own.shape[1:], jnp.float32)
    return (own + strength * shared) * lax.rsqrt(1 + strength * strength)


def setup_inputs(seed: int = 0, part: int = 0) -> dict:
    kx, kdy, ka, kb, kz, kf, kh, kl, *keys = jax.random.split(jax.random.key(seed), 8 + 3 * len(NAMES))
    kx, kdy, ka, kb = (jax.random.fold_in(k, part) for k in (kx, kdy, ka, kb))
    kw, km, kv = (keys[i::3] for i in range(3))
    shape = (SEQUENCES, TOKENS, D)
    much_x, much_dy = jax.random.uniform(kz, (2,), jnp.float32, 0.0, 1.0)
    loud = 2.0 ** jax.random.uniform(jax.random.fold_in(kz, 1), (), jnp.float32, -1.0, 2.0)
    layers = 2.0 ** jax.random.uniform(kl, (LAYERS, 1, 1), jnp.float32, -1.0, 1.0)
    x = together(ka, jax.random.normal(kx, shape, jnp.float32), much_x) * bump(kf, D, 4.0)
    dy = together(kb, jax.random.normal(kdy, shape, jnp.float32), much_dy)
    drawn = {"x": x.astype(jnp.bfloat16), "dy": (loud * dy * (SEQUENCES * TOKENS) ** -0.5).astype(jnp.bfloat16)}
    for key, name in zip(kw, NAMES, strict=True):
        w = jax.random.normal(key, SHAPES[name], jnp.float32) * SHAPES[name][1] ** -0.5
        drawn[name] = (w * {"w_gate": 1.0, "w_up": bump(kh, FF, 4.0), "w_down": layers}[name]).astype(jnp.bfloat16)
    for key, name in zip(km, NAMES, strict=True):
        drawn[f"m_{name}"] = 0.1 * jax.random.normal(key, SHAPES[name], jnp.float32)
    for key, name in zip(kv, NAMES, strict=True):
        drawn[f"v_{name}"] = jax.random.uniform(key, SHAPES[name], jnp.float32, 0.005, 0.015)
    return drawn


def matmul(a, w):
    return jnp.dot(a, w, preferred_element_type=jnp.float32).astype(jnp.bfloat16)


def normed(h):
    wide = h.astype(jnp.float32)
    scale = lax.rsqrt(jnp.mean(wide**2, -1, keepdims=True) + 1e-6)
    return (wide * scale).astype(jnp.bfloat16)


def layer(h, w):
    a = normed(h)
    gate = jnp.dot(a, w["w_gate"], preferred_element_type=jnp.float32)
    up = jnp.dot(a, w["w_up"], preferred_element_type=jnp.float32)
    return h + matmul((jax.nn.silu(gate) * up).astype(jnp.bfloat16), w["w_down"])


def adamw(w, m, v, g):
    m = 0.9 * m + 0.1 * g
    v = 0.95 * v + 0.05 * g * g
    step = m * lax.rsqrt(v + 1e-8) + 0.1 * w
    return (w - 0.02 * step).astype(jnp.bfloat16), m, v


def clipped(gradients, sum_of_squares, count):
    factor = jnp.minimum(1.0, 0.5 * lax.rsqrt(sum_of_squares / count + 1e-30))
    return [g * factor for g in gradients]


def stack(weights, h):
    return lax.scan(lambda h, w: (layer(h, w), None), h, weights)[0]


def reference(x, dy, w_gate, w_up, w_down, m_w_gate, m_w_up, m_w_down, v_w_gate, v_w_up, v_w_down):
    weights = dict(zip(NAMES, (w_gate, w_up, w_down), strict=True))

    def take(so_far, sequence):
        h, by_y = sequence
        _, back = jax.vjp(lambda w: stack(w, h), weights)
        return jax.tree.map(lambda total, term: total + term.astype(jnp.float32), so_far, back(by_y)[0]), None

    none_yet = {name: jnp.zeros(w.shape, jnp.float32) for name, w in weights.items()}
    by_weights, _ = lax.scan(take, none_yet, (x, dy))
    gradients = [by_weights[name].astype(jnp.bfloat16).astype(jnp.float32) for name in NAMES]
    gradients = clipped(gradients, sum(jnp.sum(g * g) for g in gradients), sum(g.size for g in gradients))
    new = [
        adamw(w.astype(jnp.float32), m, v, g)
        for w, m, v, g in zip((w_gate, w_up, w_down), (m_w_gate, m_w_up, m_w_down), (v_w_gate, v_w_up, v_w_down), gradients, strict=True)
    ]
    return tuple(one[which] for which in range(3) for one in new)
```

```python
import functools

import jax
import jax.numpy as jnp
from jax import lax
from jax.experimental import pallas as pl
from jax.experimental.pallas import tpu as pltpu
from jax.sharding import PartitionSpec as P

MESH = pl.DeviceIdType.MESH
CHIPS = 4
PARTS = 8
F32, BF16 = jnp.float32, jnp.bfloat16


def dot(a, b):
    return jnp.dot(a, b, preferred_element_type=F32)


def dot_nt(a, b):
    return lax.dot_general(a, b, (((1,), (1,)), ((), ())), preferred_element_type=F32)


def inverse_size(wide):
    return lax.rsqrt(jnp.mean(wide * wide, -1, keepdims=True) + 1e-6)


def gradients_kernel(
    sizes,
    x_ref, dy_ref, wg_ref, wu_ref, wd_ref,
    g_ref, own_ref, pair_ref, chain_ref, ssq_ref, h_ref,
    a, at, up, upt, acc, wgu, wd, hid, dgu, gb, st, out, ssq,
    w_sem, io_sem, pair_send, own_sem, pair_recv, ld_sem, chain_send, chain_recv, fin_sem, pass_send, pass_recv, mate_send, mate_recv, ssq_send, ssq_recv,
):
    T, D, FS, RT, RD = sizes
    NS = 2 * PARTS
    half, quarter = D // 2, D // 4
    dp = lax.axis_index("dp")
    z, c = dp // 2, dp % 2
    mate = dp + 1 - 2 * c
    last = CHIPS - 1

    barrier = pltpu.get_barrier_semaphore()
    for k in range(1, 2 * CHIPS):
        pl.semaphore_signal(barrier, inc=1, device_id={"dp": (dp + k) % (2 * CHIPS)}, device_id_type=MESH)

    def weight_copies(w):
        layer = jnp.where((w >= PARTS) & (w < 2 * PARTS), 1, 0)
        columns = pl.ds(pl.multiple_of((w % PARTS) * FS, FS), FS)
        slot = w % 2
        return (
            pltpu.make_async_copy(wg_ref.at[layer, :, columns], wgu.at[slot, :, pl.ds(0, FS)], w_sem.at[slot, 0]),
            pltpu.make_async_copy(wu_ref.at[layer, :, columns], wgu.at[slot, :, pl.ds(FS, FS)], w_sem.at[slot, 1]),
            pltpu.make_async_copy(wd_ref.at[layer, columns, :], wd.at[slot], w_sem.at[slot, 2]),
        )

    def fetch(w):
        for copy in weight_copies(w):
            copy.start()

    def fetched(w):
        for copy in weight_copies(w):
            copy.wait()

    def rows_of(r, size):
        return pl.ds(pl.multiple_of(r * size, size), size)

    def over_rows(total, size, body):
        lax.fori_loop(0, total // size, lambda r, _: (body(rows_of(r, size)), 0)[1], 0)

    fetch(0)
    load_x = pltpu.make_async_copy(x_ref.at[0], a, io_sem.at[0])
    load_x.start()
    load_x2 = pltpu.make_async_copy(x_ref.at[0], up, io_sem.at[1])
    load_x2.start()
    ssq[...] = jnp.zeros_like(ssq)
    load_x.wait()

    def norm_in_place(rows):
        wide = a[rows, :].astype(F32)
        a[rows, :] = (wide * inverse_size(wide)).astype(BF16)

    over_rows(T, RD, norm_in_place)

    def forward(j, _):
        slot = j % 2
        fetched(j)
        fetch(j + 1)

        def tile(rows):
            gu = dot(a[rows, :], wgu[slot])
            gate, lift = gu[:, :FS], gu[:, FS:]
            hidden = (gate * jax.nn.sigmoid(gate) * lift).astype(BF16)
            acc[rows, :] = jnp.where(j > 0, acc[rows, :], 0.0) + dot(hidden, wd[slot])

        over_rows(T, RT, tile)
        return 0

    lax.fori_loop(0, PARTS, forward, 0)

    load_x2.wait()

    def close_forward(rows):
        h = up[rows, :].astype(F32) + acc[rows, :].astype(BF16).astype(F32)
        h = h.astype(BF16)
        up[rows, :] = h
        wide = h.astype(F32)
        a[rows, :] = (wide * inverse_size(wide)).astype(BF16)
        acc[rows, :] = jnp.zeros((RD, D), F32)

    over_rows(T, RD, close_forward)
    save_h = pltpu.make_async_copy(up, h_ref, io_sem.at[0])
    save_h.start()

    def turn(source, target):
        def tile(rows):
            target[:, rows] = source[rows, :].T

        over_rows(T, RD, tile)

    turn(a, at)
    save_h.wait()
    load_dy = pltpu.make_async_copy(dy_ref.at[0], up, io_sem.at[1])
    load_dy.start()
    load_dy.wait()
    turn(up, upt)

    pl.semaphore_wait(barrier, 2 * CHIPS - 1)

    def cross_layers():
        load_h = pltpu.make_async_copy(h_ref, dgu, io_sem.at[0])
        load_h.start()
        again = pltpu.make_async_copy(x_ref.at[0], a, io_sem.at[1])
        again.start()
        load_h.wait()

        def tile(rows):
            wide = dgu[rows, :].astype(F32)
            scale = inverse_size(wide)
            da = acc[rows, :].astype(BF16).astype(F32)
            along = jnp.sum(da * wide, -1, keepdims=True) * (1.0 / D)
            dh = (scale * da - wide * (scale * scale * scale * along)).astype(BF16)
            up[rows, :] = (up[rows, :].astype(F32) + dh.astype(F32)).astype(BF16)

        over_rows(T, RD, tile)
        again.wait()
        over_rows(T, RD, norm_in_place)
        turn(a, at)
        turn(up, upt)

    def mine(rows_half):
        return pl.ds(pl.multiple_of(rows_half * half, half), half)

    def pair_copy(i):
        return pltpu.make_async_remote_copy(
            src_ref=gb.at[i % 2, :, mine(1 - c), :], dst_ref=pair_ref.at[i], send_sem=pair_send.at[i % 2], recv_sem=pair_recv.at[i],
            device_id={"dp": mate}, device_id_type=MESH,
        )

    def own_copy(i):
        return pltpu.make_async_copy(gb.at[i % 2, :, mine(c), :], own_ref.at[i], own_sem.at[i % 2])

    class Way:
        def __init__(self, d):
            self.d = d
            self.place = z if d == 0 else last - z
            self.step = 2 if d == 0 else -2
            self.small = pl.ds(d * quarter, quarter)
            self.rows = pl.ds(pl.multiple_of((2 * c + d) * quarter, quarter), quarter)

        def loads(self, i):
            d = self.d
            return (
                pltpu.make_async_copy(own_ref.at[i, :, self.small, :], st.at[d, 0], ld_sem.at[d, 0]),
                pltpu.make_async_copy(pair_ref.at[i, :, self.small, :], st.at[d, 1], ld_sem.at[d, 1]),
                pltpu.make_async_copy(chain_ref.at[d, i], st.at[d, 2], ld_sem.at[d, 2]),
            )

        def hop(self, i):
            d = self.d
            return pltpu.make_async_remote_copy(
                src_ref=out.at[d, i % 2], dst_ref=chain_ref.at[d, i], send_sem=chain_send.at[d, i % 2], recv_sem=chain_recv.at[d, i],
                device_id={"dp": (dp + self.step) % (2 * CHIPS)}, device_id_type=MESH,
            )

        def keep(self, i):
            return pltpu.make_async_copy(out.at[self.d, i % 2], g_ref.at[i, :, self.rows, :], fin_sem.at[i % 2])

        def spread(self, i):
            return pltpu.make_async_remote_copy(
                src_ref=g_ref.at[i, :, self.rows, :], dst_ref=g_ref.at[i, :, self.rows, :], send_sem=pass_send.at[self.d, i], recv_sem=pass_recv.at[self.d, i],
                device_id={"dp": (dp - self.step + 2 * CHIPS) % (2 * CHIPS)}, device_id_type=MESH,
            )

        def share(self, i):
            return pltpu.make_async_remote_copy(
                src_ref=g_ref.at[i, :, self.rows, :], dst_ref=g_ref.at[i, :, self.rows, :], send_sem=mate_send.at[self.d, i], recv_sem=mate_recv.at[self.d, i],
                device_id={"dp": mate}, device_id_type=MESH,
            )

    ways = (Way(0), Way(1))

    def inside(i):
        return (i >= 0) & (i < NS)

    def start_hops(t):
        @pl.when(inside(t - 1))
        def _():
            pair_copy(t - 1).wait()
            own_copy(t - 1).wait()

        for way in ways:
            i = t - 1 - way.place

            @pl.when(inside(i))
            def _():
                own, pair, chain = way.loads(i)
                own.start()
                pair.start()

                @pl.when(way.place > 0)
                def _():
                    way.hop(i).wait_recv()
                    chain.start()

    def finish_hops(t):
        for way in ways:
            d = way.d
            i = t - 1 - way.place

            @pl.when(inside(i))
            def _():
                own, pair, chain = way.loads(i)
                own.wait()
                pair.wait()

                @pl.when((way.place < last) & (i >= 2))
                def _():
                    way.hop(i - 2).wait_send()

                def piece(total, p):
                    wide = st[d, 0, p].astype(F32) + st[d, 1, p].astype(F32)
                    if total:
                        wide += st[d, 2, p].astype(F32)
                    out[d, i % 2, p] = wide.astype(BF16)

                @pl.when(way.place == 0)
                def _():
                    lax.fori_loop(0, 3, lambda p, _: (piece(False, p), 0)[1], 0)

                @pl.when(way.place > 0)
                def _():
                    chain.wait()
                    lax.fori_loop(0, 3, lambda p, _: (piece(True, p), 0)[1], 0)

                @pl.when(way.place < last)
                def _():
                    way.hop(i).start()

                @pl.when(way.place == last)
                def _():
                    way.keep(i).start()

                    def add(p, _):
                        wide = out[d, i % 2, p].astype(F32)
                        ssq[...] += jnp.sum((wide * wide).reshape(quarter // 8, 8, FS), 0)
                        return 0

                    lax.fori_loop(0, 3, add, 0)
                    way.keep(i).wait()

    def spread_sums(t):
        for way in ways:
            i = t - 1 - last - (last - way.place)

            @pl.when(inside(i))
            def _():
                @pl.when(way.place < last)
                def _():
                    way.spread(i).wait_recv()

                @pl.when(way.place > 0)
                def _():
                    way.spread(i).start()

                way.share(i).start()

    def backward(t, _):
        w = PARTS + t
        slot = w % 2
        computing = t < NS

        @pl.when(computing)
        def _():
            @pl.when(t == PARTS)
            def _():
                cross_layers()

            fetched(w)

            @pl.when(t < NS - 1)
            def _():
                fetch(w + 1)

            def tile(rows):
                gu = dot(a[rows, :], wgu[slot])
                dh = dot_nt(up[rows, :], wd[slot]).astype(BF16).astype(F32)
                gate, lift = gu[:, :FS], gu[:, FS:]
                s = jax.nn.sigmoid(gate)
                silu = gate * s
                hid[rows, :] = (silu * lift).astype(BF16)
                dgu[rows, :FS] = (dh * lift * (s + silu * (1.0 - s))).astype(BF16)
                dgu[rows, FS:] = (dh * silu).astype(BF16)

            over_rows(T, RT, tile)

        start_hops(t)

        @pl.when(computing)
        def _():
            def tile(k, _):
                rows = mine(jnp.where(k == 0, 1 - c, c))
                gb[t % 2, 2, rows, :] = dot(upt[rows, :], hid[...]).astype(BF16)
                return 0

            lax.fori_loop(0, 2, tile, 0)

        finish_hops(t)

        @pl.when(computing)
        def _():
            def tile(k, _):
                rows = mine(jnp.where(k == 0, 1 - c, c))
                both = dot(at[rows, :], dgu[...]).astype(BF16)
                gb[t % 2, 0, rows, :] = both[:, :FS]
                gb[t % 2, 1, rows, :] = both[:, FS:]
                return 0

            lax.fori_loop(0, 2, tile, 0)
            pair_copy(t).start()
            own_copy(t).start()

        spread_sums(t)

        @pl.when(t < PARTS)
        def _():
            def tile(rows):
                acc[rows, :] += dot_nt(dgu[rows, :], wgu[slot])

            over_rows(T, RT, tile)

        return 0

    lax.fori_loop(0, NS + 2 * CHIPS - 1, backward, 0)

    for at_end in range(2):
        way = ways[1 - at_end]
        for core in range(2):
            slot = 2 * at_end + core
            holder = 2 * last * at_end + core

            def to(k, slot=slot):
                return pltpu.make_async_remote_copy(
                    src_ref=ssq, dst_ref=ssq_ref.at[slot], send_sem=ssq_send.at[k], recv_sem=ssq_recv.at[slot],
                    device_id={"dp": (dp + k) % (2 * CHIPS)}, device_id_type=MESH,
                )

            local = pltpu.make_async_copy(ssq, ssq_ref.at[slot], io_sem.at[0])

            @pl.when(dp == holder)
            def _():
                local.start()
                for k in range(1, 2 * CHIPS):
                    to(k).start()
                local.wait()
                for k in range(1, 2 * CHIPS):
                    to(k).wait_send()

            @pl.when(dp != holder)
            def _():
                to(0).wait_recv()

    for way in ways:

        @pl.when(way.place < last)
        def _():
            way.hop(NS - 2).wait_send()
            way.hop(NS - 1).wait_send()

        def close(i, _):
            @pl.when(way.place > 0)
            def _():
                way.spread(i).wait_send()

            way.share(i).wait()
            return 0

        lax.fori_loop(0, NS, close, 0)


def gradients(x, dy, w_gate, w_up, w_down):
    _, T, D = x.shape
    F = w_gate.shape[2]
    FS = F // PARTS
    RT, RD = min(512, T), min(256, T)
    NS = 2 * PARTS
    anywhere = pl.BlockSpec(memory_space=pl.ANY)
    dma = pltpu.SemaphoreType.DMA
    return pl.pallas_call(
        functools.partial(gradients_kernel, (T, D, FS, RT, RD)),
        out_shape=(
            jax.ShapeDtypeStruct((NS, 3, D, FS), BF16),
            jax.ShapeDtypeStruct((NS, 3, D // 2, FS), BF16),
            jax.ShapeDtypeStruct((NS, 3, D // 2, FS), BF16),
            jax.ShapeDtypeStruct((2, NS, 3, D // 4, FS), BF16),
            jax.ShapeDtypeStruct((4, 8, FS), F32),
            jax.ShapeDtypeStruct((T, D), BF16),
        ),
        in_specs=[anywhere] * 5,
        out_specs=(anywhere,) * 6,
        scratch_shapes=[
            pltpu.VMEM((T, D), BF16),
            pltpu.VMEM((D, T), BF16),
            pltpu.VMEM((T, D), BF16),
            pltpu.VMEM((D, T), BF16),
            pltpu.VMEM((T, D), F32),
            pltpu.VMEM((2, D, 2 * FS), BF16),
            pltpu.VMEM((2, FS, D), BF16),
            pltpu.VMEM((T, FS), BF16),
            pltpu.VMEM((T, 2 * FS), BF16),
            pltpu.VMEM((2, 3, D, FS), BF16),
            pltpu.VMEM((2, 3, 3, D // 4, FS), BF16),
            pltpu.VMEM((2, 2, 3, D // 4, FS), BF16),
            pltpu.VMEM((8, FS), F32),
            dma((2, 3)),
            dma((2,)),
            dma((2,)),
            dma((2,)),
            dma((NS,)),
            dma((2, 3)),
            dma((2, 2)),
            dma((2, NS)),
            dma((2,)),
            dma((2, NS)),
            dma((2, NS)),
            dma((2, NS)),
            dma((2, NS)),
            dma((2 * CHIPS,)),
            dma((4,)),
        ],
        compiler_params=pltpu.CompilerParams(collective_id=0, has_side_effects=True, vmem_limit_bytes=66_000_000),
        name="gradients",
    )(x, dy, w_gate, w_up, w_down)


def adamw_kernel(count, ssq_ref, g_ref, *refs):
    ins, outs = refs[:9], refs[9:]
    factor = jnp.minimum(1.0, 0.5 * lax.rsqrt(jnp.sum(ssq_ref[...]) / count + 1e-30))
    for k in range(3):
        w_ref, m_ref, v_ref = ins[k::3]
        g = g_ref[0, k].astype(F32)
        if k == 2:
            g = g.T
        g = g * factor
        m = 0.9 * m_ref[0] + 0.1 * g
        v = 0.95 * v_ref[0] + 0.05 * g * g
        w = w_ref[0].astype(F32)
        outs[k][0] = (w - 0.02 * (m * lax.rsqrt(v + 1e-8) + 0.1 * w)).astype(BF16)
        outs[3 + k][0] = m
        outs[6 + k][0] = v


def adamw(ssq, g, arrays):
    NS, _, D, FS = g.shape
    rows = min(256, D)

    def across(i, r):
        return 1 - i // PARTS, r, i % PARTS

    def down(i, r):
        return 1 - i // PARTS, i % PARTS, r

    specs = [pl.BlockSpec((1, rows, FS), across), pl.BlockSpec((1, rows, FS), across), pl.BlockSpec((1, FS, rows), down)] * 3
    count = 3 * g.shape[0] * D * FS
    return pl.pallas_call(
        functools.partial(adamw_kernel, float(count)),
        grid=(NS, D // rows),
        in_specs=[pl.BlockSpec(ssq.shape, lambda i, r: (0, 0, 0)), pl.BlockSpec((1, 3, rows, FS), lambda i, r: (i, 0, r, 0))] + specs,
        out_specs=specs,
        out_shape=[jax.ShapeDtypeStruct(a.shape, a.dtype) for a in arrays],
        compiler_params=pltpu.CompilerParams(dimension_semantics=("arbitrary", "arbitrary"), vmem_limit_bytes=50_000_000),
        name="adamw",
    )(ssq, g, *arrays)


def solution(mesh):
    def step(x, dy, *arrays):
        g, *_, ssq, _ = gradients(x, dy, *arrays[:3])
        return tuple(adamw(ssq, g, arrays))

    return jax.shard_map(
        step,
        mesh=mesh,
        in_specs=(P(("rep", "dp"), None, None),) * 2 + (P(None, None, None),) * 9,
        out_specs=(P("rep", None, None),) * 9,
        check_vma=False,
    )
```

```python
import functools

import jax
import jax.numpy as jnp
from jax import lax
from jax.experimental import pallas as pl
from jax.experimental.pallas import tpu as pltpu
from jax.sharding import PartitionSpec as P


MESH = pl.DeviceIdType.MESH
CHIPS = 4
PARTS = 8
NS = 2 * PARTS
WHOLE = 4
LAG = 3
SLOTS = 4
F32, BF16 = jnp.float32, jnp.bfloat16


def dot(a, b):
    return jnp.dot(a, b, preferred_element_type=F32)


def dot_nt(a, b):
    return lax.dot_general(a, b, (((1,), (1,)), ((), ())), preferred_element_type=F32)


def inverse_size(wide):
    return lax.rsqrt(jnp.mean(wide * wide, -1, keepdims=True) + 1e-6)


def gradients_kernel(
    sizes,
    x_ref, dy_ref, wg_ref, wu_ref, wd_ref,
    g_ref, own_ref, pair_ref, chain_ref, ssq_ref, h_ref,
    a, at, up, upt, acc, wgu, wd, hid, dgu, gb, st, out, ssq,
    w_sem, io_sem, pair_send, own_sem, pair_recv, ld_sem, chain_send, chain_recv, keep_sem, pass_send, pass_recv, mate_send, mate_recv, ssq_send, ssq_recv,
):
    T, D, FS, RT, RD = sizes
    UNITS = 3 * NS
    half, quarter = D // 2, D // 4
    dp = lax.axis_index("dp")
    z, c = dp // 2, dp % 2
    mate = dp + 1 - 2 * c
    last = CHIPS - 1

    barrier = pltpu.get_barrier_semaphore()
    for k in range(1, 2 * CHIPS):
        pl.semaphore_signal(barrier, inc=1, device_id={"dp": (dp + k) % (2 * CHIPS)}, device_id_type=MESH)

    def weight_copies(w):
        layer = jnp.where((w >= PARTS) & (w < 2 * PARTS), 1, 0)
        columns = pl.ds(pl.multiple_of((w % PARTS) * FS, FS), FS)
        slot = w % 2
        return (
            pltpu.make_async_copy(wg_ref.at[layer, :, columns], wgu.at[slot, :, pl.ds(0, FS)], w_sem.at[slot, 0]),
            pltpu.make_async_copy(wu_ref.at[layer, :, columns], wgu.at[slot, :, pl.ds(FS, FS)], w_sem.at[slot, 1]),
            pltpu.make_async_copy(wd_ref.at[layer, columns, :], wd.at[slot], w_sem.at[slot, 2]),
        )

    def fetch(w):
        for copy in weight_copies(w):
            copy.start()

    def fetched(w):
        for copy in weight_copies(w):
            copy.wait()

    def rows_of(r, size):
        return pl.ds(pl.multiple_of(r * size, size), size)

    def repeat(n, body):
        lax.fori_loop(0, n, lambda r, _: (body(r), 0)[1], 0)

    def over_rows(total, size, body):
        repeat(total // size, lambda r: body(rows_of(r, size)))

    load_x = pltpu.make_async_copy(x_ref.at[0], a, io_sem.at[0])
    load_x.start()
    fetch(0)
    load_again = pltpu.make_async_copy(x_ref.at[0], dgu, io_sem.at[1])
    load_again.start()
    load_dy = pltpu.make_async_copy(dy_ref.at[0], up, io_sem.at[2])
    load_dy.start()
    ssq[...] = jnp.zeros_like(ssq)
    load_x.wait()

    def norm_in_place(rows):
        wide = a[rows, :].astype(F32)
        a[rows, :] = (wide * inverse_size(wide)).astype(BF16)

    over_rows(T, RD, norm_in_place)

    def forward(j):
        slot = j % 2
        fetched(j)
        fetch(j + 1)

        def tile(rows):
            gu = dot(a[rows, :], wgu[slot])
            gate, lift = gu[:, :FS], gu[:, FS:]
            hidden = (gate * jax.nn.sigmoid(gate) * lift).astype(BF16)
            acc[rows, :] = jnp.where(j > 0, acc[rows, :], 0.0) + dot(hidden, wd[slot])

        over_rows(T, RT, tile)

    repeat(PARTS, forward)

    load_again.wait()

    def close_forward(rows):
        h = dgu[rows, :].astype(F32) + acc[rows, :].astype(BF16).astype(F32)
        h = h.astype(BF16)
        dgu[rows, :] = h
        wide = h.astype(F32)
        a[rows, :] = (wide * inverse_size(wide)).astype(BF16)
        acc[rows, :] = jnp.zeros((RD, D), F32)

    over_rows(T, RD, close_forward)
    save_h = pltpu.make_async_copy(dgu, h_ref, io_sem.at[0])
    save_h.start()

    def turn(source, target):
        def tile(rows):
            target[:, rows] = source[rows, :].T

        over_rows(T, RD, tile)

    load_dy.wait()
    turn(a, at)
    turn(up, upt)
    save_h.wait()
    pl.semaphore_wait(barrier, 2 * CHIPS - 1)

    reload_x = pltpu.make_async_copy(x_ref.at[0], a, io_sem.at[1])

    def cross_layers():
        load_h = pltpu.make_async_copy(h_ref, dgu, io_sem.at[0])
        load_h.start()
        reload_x.wait()
        over_rows(T, RD, norm_in_place)
        turn(a, at)
        load_h.wait()

        def tile(rows):
            wide = dgu[rows, :].astype(F32)
            scale = inverse_size(wide)
            da = acc[rows, :].astype(BF16).astype(F32)
            along = jnp.sum(da * wide, -1, keepdims=True) * (1.0 / D)
            dh = (scale * da - wide * (scale * scale * scale * along)).astype(BF16)
            up[rows, :] = (up[rows, :].astype(F32) + dh.astype(F32)).astype(BF16)

        over_rows(T, RD, tile)
        turn(up, upt)

    def half_of(core):
        return pl.ds(pl.multiple_of(core * half, half), half)

    def pair_copy(n):
        i, p = n // 3, n % 3
        return pltpu.make_async_remote_copy(
            src_ref=gb.at[i % 2, p, half_of(1 - c), :], dst_ref=pair_ref.at[i, p], send_sem=pair_send.at[i % 2, p], recv_sem=pair_recv.at[i, p],
            device_id={"dp": mate}, device_id_type=MESH,
        )

    def own_copy(n):
        i, p = n // 3, n % 3
        return pltpu.make_async_copy(gb.at[i % 2, p, half_of(c), :], own_ref.at[i, p], own_sem.at[i % 2, p])

    class Way:
        def __init__(self, d):
            self.d = d
            self.place = z if d == 0 else last - z
            self.step = 2 if d == 0 else -2
            self.small = pl.ds(d * quarter, quarter)
            self.rows = pl.ds(pl.multiple_of((2 * c + d) * quarter, quarter), quarter)

        def loads(self, n):
            d, i, p = self.d, n // 3, n % 3
            return (
                pltpu.make_async_copy(own_ref.at[i, p, self.small, :], st.at[d, 0], ld_sem.at[d, 0]),
                pltpu.make_async_copy(pair_ref.at[i, p, self.small, :], st.at[d, 1], ld_sem.at[d, 1]),
                pltpu.make_async_copy(chain_ref.at[d, i, p], st.at[d, 2], ld_sem.at[d, 2]),
            )

        def hop(self, n):
            d, i, p = self.d, n // 3, n % 3
            return pltpu.make_async_remote_copy(
                src_ref=out.at[d, n % SLOTS], dst_ref=chain_ref.at[d, i, p], send_sem=chain_send.at[d, n % SLOTS], recv_sem=chain_recv.at[d, i, p],
                device_id={"dp": (dp + self.step) % (2 * CHIPS)}, device_id_type=MESH,
            )

        def keep(self, n):
            return pltpu.make_async_copy(out.at[self.d, n % SLOTS], g_ref.at[n // 3, n % 3, self.rows, :], keep_sem.at[n % SLOTS])

        def spread(self, n):
            d, i, p = self.d, n // 3, n % 3
            return pltpu.make_async_remote_copy(
                src_ref=g_ref.at[i, p, self.rows, :], dst_ref=g_ref.at[i, p, self.rows, :], send_sem=pass_send.at[d, i, p], recv_sem=pass_recv.at[d, i, p],
                device_id={"dp": (dp - self.step + 2 * CHIPS) % (2 * CHIPS)}, device_id_type=MESH,
            )

        def share(self, n):
            d, i, p = self.d, n // 3, n % 3
            return pltpu.make_async_remote_copy(
                src_ref=g_ref.at[i, p, self.rows, :], dst_ref=g_ref.at[i, p, self.rows, :], send_sem=mate_send.at[d, i, p], recv_sem=mate_recv.at[d, i, p],
                device_id={"dp": mate}, device_id_type=MESH,
            )

        def reaches(self, n, place):
            return last - place <= WHOLE + last - 1 - n // 3

        def holds(self, n):
            return (self.place == last) | self.reaches(n, self.place)

        def passes(self, n):
            return (self.place > 0) & self.reaches(n, self.place - 1)

    ways = (Way(0), Way(1))

    def inside(n):
        return (n >= 0) & (n < UNITS)

    def start_tick(k):
        @pl.when(inside(k - 2))
        def _():
            own_copy(k - 2).wait()
            pair_copy(k - 2).wait_recv()

        for way in ways:
            n = k - 2 - LAG * way.place

            @pl.when(inside(n))
            def _(way=way, n=n):
                own, pair, chain = way.loads(n)
                own.start()
                pair.start()

                @pl.when(way.place > 0)
                def _():
                    way.hop(n).wait_recv()
                    chain.start()

    def finish_tick(k):
        for way in ways:
            d = way.d
            n = k - 2 - LAG * way.place

            @pl.when(inside(n))
            def _(way=way, d=d, n=n):
                own, pair, chain = way.loads(n)
                own.wait()
                pair.wait()

                @pl.when((way.place < last) & (n >= SLOTS))
                def _():
                    way.hop(n - SLOTS).wait_send()

                def add(so_far):
                    wide = st[d, 0].astype(F32) + st[d, 1].astype(F32)
                    if so_far:
                        wide += st[d, 2].astype(F32)
                    rounded = wide.astype(BF16)
                    out[d, n % SLOTS] = rounded
                    return rounded.astype(F32)

                @pl.when(way.place == 0)
                def _():
                    add(False)
                    way.hop(n).start()

                @pl.when((way.place > 0) & (way.place < last))
                def _():
                    chain.wait()
                    add(True)
                    way.hop(n).start()

                @pl.when(way.place == last)
                def _():
                    chain.wait()
                    total = add(True)
                    way.keep(n).start()
                    ssq[...] += jnp.sum((total * total).reshape(quarter // 8, 8, FS), 0)

        for way in ways:
            n = k - 3 - LAG * (2 * last - way.place)

            @pl.when(inside(n))
            def _(way=way, n=n):
                @pl.when(way.place == last)
                def _():
                    way.keep(n).wait()

                @pl.when((way.place < last) & way.holds(n))
                def _():
                    way.spread(n).wait_recv()

                @pl.when(way.passes(n))
                def _():
                    way.spread(n).start()

                @pl.when(way.holds(n))
                def _():
                    way.share(n).start()

    def backward(t):
        w = PARTS + t
        slot = w % 2

        @pl.when(t == PARTS)
        def _():
            cross_layers()

        fetched(w)

        @pl.when(t < NS - 1)
        def _():
            fetch(w + 1)

        def hidden_half(k):
            start_tick(3 * t + k)

            def tile(r):
                rows = rows_of(k * (T // RT // 2) + r, RT)
                gu = dot(a[rows, :], wgu[slot])
                dh = dot_nt(up[rows, :], wd[slot]).astype(BF16).astype(F32)
                gate, lift = gu[:, :FS], gu[:, FS:]
                s = jax.nn.sigmoid(gate)
                silu = gate * s
                hid[rows, :] = (silu * lift).astype(BF16)
                dgu[rows, :FS] = (dh * lift * (s + silu * (1.0 - s))).astype(BF16)
                dgu[rows, FS:] = (dh * silu).astype(BF16)

            repeat(T // RT // 2, tile)
            finish_tick(3 * t + k)

        repeat(2, hidden_half)

        @pl.when(t == PARTS - 1)
        def _():
            reload_x.start()

        @pl.when(t >= 2)
        def _():
            for p in range(3):
                pair_copy(3 * (t - 2) + p).wait_send()

        def down_half(k):
            rows = half_of(jnp.where(k == 0, 1 - c, c))
            gb[t % 2, 0, rows, :] = dot(upt[rows, :], hid[...]).astype(BF16)

            @pl.when(k == 0)
            def _():
                pair_copy(3 * t).start()

            @pl.when(k == 1)
            def _():
                own_copy(3 * t).start()

        repeat(2, down_half)

        def both_half(k):
            @pl.when(k == 1)
            def _():
                start_tick(3 * t + 2)

            rows = half_of(jnp.where(k == 0, 1 - c, c))
            both = dot(at[rows, :], dgu[...]).astype(BF16)
            gb[t % 2, 1, rows, :] = both[:, :FS]
            gb[t % 2, 2, rows, :] = both[:, FS:]

            @pl.when(k == 0)
            def _():
                pair_copy(3 * t + 1).start()
                pair_copy(3 * t + 2).start()

            @pl.when(k == 1)
            def _():
                own_copy(3 * t + 1).start()
                own_copy(3 * t + 2).start()
                finish_tick(3 * t + 2)

        repeat(2, both_half)

        @pl.when(t < PARTS)
        def _():
            def tile(rows):
                acc[rows, :] += dot_nt(dgu[rows, :], wgu[slot])

            over_rows(T, RT, tile)

    repeat(NS, backward)

    def drain(k):
        start_tick(UNITS + k)
        finish_tick(UNITS + k)

    ticks = max(UNITS + 2 + LAG * last + 1, 3 * (WHOLE + last - 1) + 2 + LAG * 2 * last + 1)
    repeat(ticks - UNITS, drain)

    for at_end in range(2):
        for core in range(2):
            slot = 2 * at_end + core
            holder = 2 * last * at_end + core

            def to(k, slot=slot):
                return pltpu.make_async_remote_copy(
                    src_ref=ssq, dst_ref=ssq_ref.at[slot], send_sem=ssq_send.at[k], recv_sem=ssq_recv.at[slot],
                    device_id={"dp": (dp + k) % (2 * CHIPS)}, device_id_type=MESH,
                )

            local = pltpu.make_async_copy(ssq, ssq_ref.at[slot], io_sem.at[0])

            @pl.when(dp == holder)
            def _(to=to, local=local):
                local.start()
                for k in range(1, 2 * CHIPS):
                    to(k).start()
                local.wait()
                for k in range(1, 2 * CHIPS):
                    to(k).wait_send()

    for slot in range(4):
        holder = 2 * last * (slot // 2) + slot % 2

        @pl.when(dp != holder)
        def _(slot=slot):
            pltpu.make_async_remote_copy(
                src_ref=ssq, dst_ref=ssq_ref.at[slot], send_sem=ssq_send.at[0], recv_sem=ssq_recv.at[slot],
                device_id={"dp": dp}, device_id_type=MESH,
            ).wait_recv()

    for p in range(3):
        pair_copy(3 * (NS - 2) + p).wait_send()
        pair_copy(3 * (NS - 1) + p).wait_send()

    for way in ways:

        @pl.when(way.place < last)
        def _(way=way):
            repeat(SLOTS, lambda k: way.hop(UNITS - SLOTS + k).wait_send())

        def close(n, way=way):
            @pl.when(way.passes(n))
            def _():
                way.spread(n).wait_send()

            @pl.when(way.holds(n))
            def _():
                way.share(n).wait()

        repeat(UNITS, close)


def gradients(x, dy, w_gate, w_up, w_down):
    _, T, D = x.shape
    F = w_gate.shape[2]
    FS = F // PARTS
    RT, RD = min(512, T // 2), min(256, T)
    anywhere = pl.BlockSpec(memory_space=pl.ANY)
    dma = pltpu.SemaphoreType.DMA
    return pl.pallas_call(
        functools.partial(gradients_kernel, (T, D, FS, RT, RD)),
        out_shape=(
            jax.ShapeDtypeStruct((NS, 3, D, FS), BF16),
            jax.ShapeDtypeStruct((NS, 3, D // 2, FS), BF16),
            jax.ShapeDtypeStruct((NS, 3, D // 2, FS), BF16),
            jax.ShapeDtypeStruct((2, NS, 3, D // 4, FS), BF16),
            jax.ShapeDtypeStruct((4, 8, FS), F32),
            jax.ShapeDtypeStruct((T, D), BF16),
        ),
        in_specs=[anywhere] * 5,
        out_specs=(anywhere,) * 6,
        scratch_shapes=[
            pltpu.VMEM((T, D), BF16),
            pltpu.VMEM((D, T), BF16),
            pltpu.VMEM((T, D), BF16),
            pltpu.VMEM((D, T), BF16),
            pltpu.VMEM((T, D), F32),
            pltpu.VMEM((2, D, 2 * FS), BF16),
            pltpu.VMEM((2, FS, D), BF16),
            pltpu.VMEM((T, FS), BF16),
            pltpu.VMEM((T, 2 * FS), BF16),
            pltpu.VMEM((2, 3, D, FS), BF16),
            pltpu.VMEM((2, 3, D // 4, FS), BF16),
            pltpu.VMEM((2, SLOTS, D // 4, FS), BF16),
            pltpu.VMEM((8, FS), F32),
            dma((2, 3)),
            dma((3,)),
            dma((2, 3)),
            dma((2, 3)),
            dma((NS, 3)),
            dma((2, 3)),
            dma((2, SLOTS)),
            dma((2, NS, 3)),
            dma((SLOTS,)),
            dma((2, WHOLE + CHIPS, 3)),
            dma((2, WHOLE + CHIPS, 3)),
            dma((2, NS, 3)),
            dma((2, NS, 3)),
            dma((2 * CHIPS,)),
            dma((4,)),
        ],
        compiler_params=pltpu.CompilerParams(collective_id=0, has_side_effects=True, vmem_limit_bytes=66_000_000),
        name="gradients",
    )(x, dy, w_gate, w_up, w_down)


def adamw_kernel(count, work, split, n_in, *refs):
    ssq_ref, g_ref = refs[:2]
    back = refs[2 : 2 + n_in]
    ins = refs[2 + n_in : 11 + n_in]
    outs, gv, sem = refs[-11:-2], refs[-2], refs[-1]
    quarter, FS = gv.shape[2:]
    dp = lax.axis_index("dp")
    z, c = dp // 2, dp % 2
    step = pl.program_id(0)

    def here(k, source):
        return pltpu.make_async_copy(source, gv.at[k], sem.at[k])

    @pl.when(step == 0)
    def _():
        for k, (i, q, came) in enumerate(work):
            whole = g_ref.at[i, :, pl.ds(q * quarter, quarter), :]
            place = z if q % 2 == 0 else CHIPS - 1 - z
            for p in range(CHIPS):
                if came[p] is None:

                    @pl.when(place == p)
                    def _(k=k, whole=whole):
                        here(k, whole).start()

                else:
                    for core in range(2):

                        @pl.when((place == p) & (c == core))
                        def _(k=k, at=came[p][0 if core == q // 2 else 1]):
                            here(k, back[at].at[0]).start()

    k, sub = step // split, step % split

    @pl.when(sub == 0)
    def _():
        here(k, g_ref.at[0, :, pl.ds(0, quarter), :]).wait()

    factor = jnp.minimum(1.0, 0.5 * lax.rsqrt(jnp.sum(ssq_ref[...]) / count + 1e-30))
    some = quarter // split

    def update(number, rows, g):
        w_ref, m_ref, v_ref = ins[number::3]
        g = g * factor
        m = 0.9 * m_ref[0, rows, :] + 0.1 * g
        v = 0.95 * v_ref[0, rows, :] + 0.05 * g * g
        w = w_ref[0, rows, :].astype(F32)
        outs[number][0, rows, :] = (w - 0.02 * (m * lax.rsqrt(v + 1e-8) + 0.1 * w)).astype(BF16)
        outs[3 + number][0, rows, :] = m
        outs[6 + number][0, rows, :] = v

    def across(r, _):
        few = some // 4
        rows = pl.ds(pl.multiple_of(r * few, few), few)
        there = pl.ds(pl.multiple_of(sub * some + r * few, few), few)
        update(0, rows, gv[k, 1, there, :].astype(F32))
        update(1, rows, gv[k, 2, there, :].astype(F32))
        return 0

    lax.fori_loop(0, 4, across, 0)

    def down(r, _):
        few = FS // 4
        rows = pl.ds(pl.multiple_of(r * few, few), few)
        update(2, rows, gv[k, 0, pl.ds(pl.multiple_of(sub * some, some), some), rows].astype(F32).T)
        return 0

    lax.fori_loop(0, 4, down, 0)


def adamw(ssq, g, arrays, results, listed, back):
    _, _, D, FS = g.shape
    quarter = D // 4
    split = 2 if quarter % 256 == 0 else 1
    some = quarter // split
    first, base = listed[0][:2], listed[-1][0]
    alone = 4 * first[0] + first[1]
    rest = 4 * base + 4 - len(listed)

    def number(s):
        k = s // split
        if all(4 * i + q == alone + at for at, (i, q, _) in enumerate(listed)):
            return alone + k
        return jnp.where(k == 0, alone, rest + k)

    def across(s):
        n = number(s)
        return 1 - n // 4 // PARTS, n % 4 * split + s % split, n // 4 % PARTS

    def down(s):
        n = number(s)
        return 1 - n // 4 // PARTS, n // 4 % PARTS, n % 4 * split + s % split

    specs = [pl.BlockSpec((1, some, FS), across), pl.BlockSpec((1, some, FS), across), pl.BlockSpec((1, FS, some), down)] * 3
    anywhere = pl.BlockSpec(memory_space=pl.ANY)
    count = 3 * g.shape[0] * D * FS
    size = 3 * len(listed) * quarter * FS
    ins = [ssq, g, *back, *arrays, *(results or ())]
    return pl.pallas_call(
        functools.partial(adamw_kernel, float(count), listed, split, len(back)),
        grid=(len(listed) * split,),
        in_specs=[pl.BlockSpec(ssq.shape, lambda s: (0, 0, 0))] + [anywhere] * (1 + len(back)) + specs + [anywhere] * (9 if results else 0),
        out_specs=specs,
        out_shape=[jax.ShapeDtypeStruct(a.shape, a.dtype) for a in arrays],
        input_output_aliases={len(ins) - 9 + k: k for k in range(9)} if results else {},
        scratch_shapes=[pltpu.VMEM((len(listed), 3, quarter, FS), BF16), pltpu.SemaphoreType.DMA((len(listed),))],
        compiler_params=pltpu.CompilerParams(dimension_semantics=("arbitrary",), vmem_limit_bytes=66_000_000),
        cost_estimate=pl.CostEstimate(flops=COST * size, bytes_accessed=22 * size, transcendentals=size),
        name="adamw",
    )(*ins)


COST = 16


def finish(g, ssq, arrays):
    _, _, D, FS = g.shape
    quarter = D // 4
    last = CHIPS - 1
    dp = lax.axis_index("dp")
    z, c = dp // 2, dp % 2
    stages = NS - WHOLE
    ready = [(i, q, (None,) * CHIPS) for i in range(WHOLE) for q in range(4)]
    back, results = [], None
    index = {}

    def kept(i, d, g=g):
        return lax.dynamic_slice(g, (jnp.asarray(i, jnp.int32), jnp.int32(0), (2 * c + d) * quarter, jnp.int32(0)), (1, 3, quarter, FS))

    def units(u):
        came = []
        for d in range(2):
            came.append(tuple(index[u - p, d] if p < last and u >= p else None for p in range(CHIPS)))
        return [(WHOLE + u, q, came[q % 2]) for q in range(4)]

    def update(results, listed):
        used = sorted({at for _, _, came in listed for pair in came if pair for at in pair})
        where = {at: k for k, at in enumerate(used)}
        listed = [(i, q, tuple(pair and tuple(where[at] for at in pair) for pair in came)) for i, q, came in listed]
        return adamw(ssq, g, arrays, results, listed, [back[at] for at in used])

    newest, pending = [None, None], []
    extra = 4 * WHOLE - 2 * 5
    for s in range(stages + 2):
        for at, swaps in pending:
            back[at + 1] = lax.ppermute(back[at], "dp", swaps)
        pending = []
        at_hand = g
        if s > 0:
            at_hand, *newest = lax.optimization_barrier((g, *newest))
        for d in range(2 if s < stages else 0):
            place = z if d == 0 else last - z
            if s == 0:
                sent = kept(WHOLE + place - 1, d)
            elif s + last - 1 < stages:
                sent = jnp.where(place == last, kept(WHOLE + s + last - 1, d, at_hand), newest[d])
            else:
                sent = newest[d]
            moves = []
            for p in range(1, CHIPS):
                if s + p - 1 < stages:
                    for core in range(2):
                        source, target = (p, p - 1) if d == 0 else (last - p, last - p + 1)
                        moves.append((2 * source + core, 2 * target + core))
            newest[d] = lax.ppermute(sent, "dp", moves)
            index[s, d] = (len(back), len(back) + 1)
            pending.append((len(back), [(to, to + 1 - 2 * (to % 2)) for _, to in moves]))
            back += [newest[d], None]
        many = 5 if s < 2 else 1 if s - 2 < extra else 0
        listed, ready = ready[:many], ready[many:]
        if s >= 2:
            listed = listed + units(s - 2)
        results = update(results, listed)
    return results


def solution(mesh):
    def step(x, dy, *arrays):
        g, *_, ssq, _ = gradients(x, dy, *arrays[:3])
        return tuple(finish(g, ssq, arrays))

    return jax.shard_map(
        step,
        mesh=mesh,
        in_specs=(P(("rep", "dp"), None, None),) * 2 + (P(None, None, None),) * 9,
        out_specs=(P("rep", None, None),) * 9,
        check_vma=False,
    )
```

```python
import functools

import jax
import jax.numpy as jnp
from jax import lax
from jax.experimental import pallas as pl
from jax.experimental.pallas import tpu as pltpu
from jax.sharding import PartitionSpec as P


MESH = pl.DeviceIdType.MESH
CHIPS = 4
PARTS = 8
NS = 2 * PARTS
WHOLE = 2
LAG = 3
SLOTS = 4
F32, BF16 = jnp.float32, jnp.bfloat16


def dot(a, b):
    return jnp.dot(a, b, preferred_element_type=F32)


def dot_nt(a, b):
    return lax.dot_general(a, b, (((1,), (1,)), ((), ())), preferred_element_type=F32)


def inverse_size(wide):
    return lax.rsqrt(jnp.mean(wide * wide, -1, keepdims=True) + 1e-6)


def gradients_kernel(
    sizes,
    x_ref, dy_ref, wg_ref, wu_ref, wd_ref,
    g_ref, own_ref, pair_ref, chain_ref, ssq_ref, h_ref,
    a, at, up, upt, acc, wgu, wd, hid, dgu, gb, st, out, ssq,
    w_sem, io_sem, pair_send, own_sem, pair_recv, ld_sem, chain_send, chain_recv, keep_sem, pass_send, pass_recv, mate_send, mate_recv, ssq_send, ssq_recv,
):
    T, D, FS, RT, RD = sizes
    UNITS = 3 * NS
    half, quarter = D // 2, D // 4
    dp = lax.axis_index("dp")
    z, c = dp // 2, dp % 2
    mate = dp + 1 - 2 * c
    last = CHIPS - 1

    barrier = pltpu.get_barrier_semaphore()
    for k in range(1, 2 * CHIPS):
        pl.semaphore_signal(barrier, inc=1, device_id={"dp": (dp + k) % (2 * CHIPS)}, device_id_type=MESH)

    def weight_copies(w):
        layer = jnp.where((w >= PARTS) & (w < 2 * PARTS), 1, 0)
        columns = pl.ds(pl.multiple_of((w % PARTS) * FS, FS), FS)
        slot = w % 2
        return (
            pltpu.make_async_copy(wg_ref.at[layer, :, columns], wgu.at[slot, :, pl.ds(0, FS)], w_sem.at[slot, 0]),
            pltpu.make_async_copy(wu_ref.at[layer, :, columns], wgu.at[slot, :, pl.ds(FS, FS)], w_sem.at[slot, 1]),
            pltpu.make_async_copy(wd_ref.at[layer, columns, :], wd.at[slot], w_sem.at[slot, 2]),
        )

    def fetch(w):
        for copy in weight_copies(w):
            copy.start()

    def fetched(w):
        for copy in weight_copies(w):
            copy.wait()

    def rows_of(r, size):
        return pl.ds(pl.multiple_of(r * size, size), size)

    def repeat(n, body):
        lax.fori_loop(0, n, lambda r, _: (body(r), 0)[1], 0)

    def over_rows(total, size, body):
        repeat(total // size, lambda r: body(rows_of(r, size)))

    load_x = pltpu.make_async_copy(x_ref.at[0], a, io_sem.at[0])
    load_x.start()
    fetch(0)
    load_again = pltpu.make_async_copy(x_ref.at[0], dgu, io_sem.at[1])
    load_again.start()
    load_dy = pltpu.make_async_copy(dy_ref.at[0], up, io_sem.at[2])
    load_dy.start()
    ssq[...] = jnp.zeros_like(ssq)
    load_x.wait()

    def norm_in_place(rows):
        wide = a[rows, :].astype(F32)
        a[rows, :] = (wide * inverse_size(wide)).astype(BF16)

    over_rows(T, RD, norm_in_place)

    def forward(j):
        slot = j % 2
        fetched(j)
        fetch(j + 1)

        def tile(rows):
            gu = dot(a[rows, :], wgu[slot])
            gate, lift = gu[:, :FS], gu[:, FS:]
            hidden = (gate * jax.nn.sigmoid(gate) * lift).astype(BF16)
            acc[rows, :] = jnp.where(j > 0, acc[rows, :], 0.0) + dot(hidden, wd[slot])

        over_rows(T, RT, tile)

    repeat(PARTS, forward)

    load_again.wait()

    def close_forward(rows):
        h = dgu[rows, :].astype(F32) + acc[rows, :].astype(BF16).astype(F32)
        h = h.astype(BF16)
        dgu[rows, :] = h
        wide = h.astype(F32)
        a[rows, :] = (wide * inverse_size(wide)).astype(BF16)
        acc[rows, :] = jnp.zeros((RD, D), F32)

    over_rows(T, RD, close_forward)
    save_h = pltpu.make_async_copy(dgu, h_ref, io_sem.at[0])
    save_h.start()

    def turn(source, target):
        def tile(rows):
            target[:, rows] = source[rows, :].T

        over_rows(T, RD, tile)

    load_dy.wait()
    turn(a, at)
    turn(up, upt)
    save_h.wait()
    pl.semaphore_wait(barrier, 2 * CHIPS - 1)

    reload_x = pltpu.make_async_copy(x_ref.at[0], a, io_sem.at[1])

    def cross_layers():
        load_h = pltpu.make_async_copy(h_ref, dgu, io_sem.at[0])
        load_h.start()
        reload_x.wait()
        over_rows(T, RD, norm_in_place)
        turn(a, at)
        load_h.wait()

        def tile(rows):
            wide = dgu[rows, :].astype(F32)
            scale = inverse_size(wide)
            da = acc[rows, :].astype(BF16).astype(F32)
            along = jnp.sum(da * wide, -1, keepdims=True) * (1.0 / D)
            dh = (scale * da - wide * (scale * scale * scale * along)).astype(BF16)
            up[rows, :] = (up[rows, :].astype(F32) + dh.astype(F32)).astype(BF16)

        over_rows(T, RD, tile)
        turn(up, upt)

    def half_of(core):
        return pl.ds(pl.multiple_of(core * half, half), half)

    def pair_copy(n):
        i, p = n // 3, n % 3
        return pltpu.make_async_remote_copy(
            src_ref=gb.at[i % 2, p, half_of(1 - c), :], dst_ref=pair_ref.at[i, p], send_sem=pair_send.at[i % 2, p], recv_sem=pair_recv.at[i, p],
            device_id={"dp": mate}, device_id_type=MESH,
        )

    def own_copy(n):
        i, p = n // 3, n % 3
        return pltpu.make_async_copy(gb.at[i % 2, p, half_of(c), :], own_ref.at[i, p], own_sem.at[i % 2, p])

    class Way:
        def __init__(self, d):
            self.d = d
            self.place = z if d == 0 else last - z
            self.step = 2 if d == 0 else -2
            self.small = pl.ds(d * quarter, quarter)
            self.block = 2 * d + c

        def loads(self, n):
            d, i, p = self.d, n // 3, n % 3
            return (
                pltpu.make_async_copy(own_ref.at[i, p, self.small, :], st.at[d, 0], ld_sem.at[d, 0]),
                pltpu.make_async_copy(pair_ref.at[i, p, self.small, :], st.at[d, 1], ld_sem.at[d, 1]),
                pltpu.make_async_copy(chain_ref.at[d, i, p], st.at[d, 2], ld_sem.at[d, 2]),
            )

        def hop(self, n):
            d, i, p = self.d, n // 3, n % 3
            return pltpu.make_async_remote_copy(
                src_ref=out.at[d, n % SLOTS], dst_ref=chain_ref.at[d, i, p], send_sem=chain_send.at[d, n % SLOTS], recv_sem=chain_recv.at[d, i, p],
                device_id={"dp": (dp + self.step) % (2 * CHIPS)}, device_id_type=MESH,
            )

        def keep(self, n):
            return pltpu.make_async_copy(out.at[self.d, n % SLOTS], g_ref.at[n // 3, n % 3, self.block], keep_sem.at[n % SLOTS])

        def spread(self, n):
            d, i, p = self.d, n // 3, n % 3
            return pltpu.make_async_remote_copy(
                src_ref=g_ref.at[i, p, self.block], dst_ref=g_ref.at[i, p, self.block], send_sem=pass_send.at[d, i, p], recv_sem=pass_recv.at[d, i, p],
                device_id={"dp": (dp - self.step + 2 * CHIPS) % (2 * CHIPS)}, device_id_type=MESH,
            )

        def share(self, n):
            d, i, p = self.d, n // 3, n % 3
            return pltpu.make_async_remote_copy(
                src_ref=g_ref.at[i, p, self.block], dst_ref=g_ref.at[i, p, self.block], send_sem=mate_send.at[d, i, p], recv_sem=mate_recv.at[d, i, p],
                device_id={"dp": mate}, device_id_type=MESH,
            )

        def reaches(self, n, place):
            return last - place <= WHOLE + last - 1 - n // 3

        def holds(self, n):
            return (self.place == last) | self.reaches(n, self.place)

        def passes(self, n):
            return (self.place > 0) & self.reaches(n, self.place - 1)

    ways = (Way(0), Way(1))

    def inside(n):
        return (n >= 0) & (n < UNITS)

    def start_tick(k):
        @pl.when(inside(k - 2))
        def _():
            own_copy(k - 2).wait()
            pair_copy(k - 2).wait_recv()

        for way in ways:
            n = k - 2 - LAG * way.place

            @pl.when(inside(n))
            def _(way=way, n=n):
                own, pair, chain = way.loads(n)
                own.start()
                pair.start()

                @pl.when(way.place > 0)
                def _():
                    way.hop(n).wait_recv()
                    chain.start()

    def finish_tick(k):
        for way in ways:
            d = way.d
            n = k - 2 - LAG * way.place

            @pl.when(inside(n))
            def _(way=way, d=d, n=n):
                own, pair, chain = way.loads(n)
                own.wait()
                pair.wait()

                @pl.when((way.place < last) & (n >= SLOTS))
                def _():
                    way.hop(n - SLOTS).wait_send()

                def add(so_far):
                    wide = st[d, 0].astype(F32) + st[d, 1].astype(F32)
                    if so_far:
                        wide += st[d, 2].astype(F32)
                    rounded = wide.astype(BF16)
                    out[d, n % SLOTS] = rounded
                    return rounded.astype(F32)

                @pl.when(way.place == 0)
                def _():
                    add(False)
                    way.hop(n).start()

                @pl.when((way.place > 0) & (way.place < last))
                def _():
                    chain.wait()
                    add(True)
                    way.hop(n).start()

                @pl.when(way.place == last)
                def _():
                    chain.wait()
                    total = add(True)
                    way.keep(n).start()
                    ssq[...] += jnp.sum((total * total).reshape(quarter // 8, 8, FS), 0)

        for way in ways:
            n = k - 3 - LAG * (2 * last - way.place)

            @pl.when(inside(n))
            def _(way=way, n=n):
                @pl.when(way.place == last)
                def _():
                    way.keep(n).wait()

                @pl.when((way.place < last) & way.holds(n))
                def _():
                    way.spread(n).wait_recv()

                @pl.when(way.passes(n))
                def _():
                    way.spread(n).start()

                @pl.when(way.holds(n))
                def _():
                    way.share(n).start()

    def backward(t):
        w = PARTS + t
        slot = w % 2

        @pl.when(t == PARTS)
        def _():
            cross_layers()

        fetched(w)

        @pl.when(t < NS - 1)
        def _():
            fetch(w + 1)

        def hidden_half(k):
            start_tick(3 * t + k)

            def tile(r):
                rows = rows_of(k * (T // RT // 2) + r, RT)
                gu = dot(a[rows, :], wgu[slot])
                dh = dot_nt(up[rows, :], wd[slot]).astype(BF16).astype(F32)
                gate, lift = gu[:, :FS], gu[:, FS:]
                s = jax.nn.sigmoid(gate)
                silu = gate * s
                hid[rows, :] = (silu * lift).astype(BF16)
                dgu[rows, :FS] = (dh * lift * (s + silu * (1.0 - s))).astype(BF16)
                dgu[rows, FS:] = (dh * silu).astype(BF16)

            repeat(T // RT // 2, tile)
            finish_tick(3 * t + k)

        repeat(2, hidden_half)

        @pl.when(t == PARTS - 1)
        def _():
            reload_x.start()

        @pl.when(t >= 2)
        def _():
            for p in range(3):
                pair_copy(3 * (t - 2) + p).wait_send()

        def down_half(k):
            rows = half_of(jnp.where(k == 0, 1 - c, c))
            gb[t % 2, 0, rows, :] = dot(upt[rows, :], hid[...]).astype(BF16)

            @pl.when(k == 0)
            def _():
                pair_copy(3 * t).start()

            @pl.when(k == 1)
            def _():
                own_copy(3 * t).start()

        repeat(2, down_half)

        def both_half(k):
            @pl.when(k == 1)
            def _():
                start_tick(3 * t + 2)

            rows = half_of(jnp.where(k == 0, 1 - c, c))
            both = dot(at[rows, :], dgu[...]).astype(BF16)
            gb[t % 2, 1, rows, :] = both[:, :FS]
            gb[t % 2, 2, rows, :] = both[:, FS:]

            @pl.when(k == 0)
            def _():
                pair_copy(3 * t + 1).start()
                pair_copy(3 * t + 2).start()

            @pl.when(k == 1)
            def _():
                own_copy(3 * t + 1).start()
                own_copy(3 * t + 2).start()
                finish_tick(3 * t + 2)

        repeat(2, both_half)

        @pl.when(t < PARTS)
        def _():
            def tile(rows):
                acc[rows, :] += dot_nt(dgu[rows, :], wgu[slot])

            over_rows(T, RT, tile)

    repeat(NS, backward)

    def drain(k):
        start_tick(UNITS + k)
        finish_tick(UNITS + k)

    ticks = max(UNITS + 2 + LAG * last + 1, 3 * (WHOLE + last - 1) + 2 + LAG * 2 * last + 1)
    repeat(ticks - UNITS, drain)

    for at_end in range(2):
        for core in range(2):
            slot = 2 * at_end + core
            holder = 2 * last * at_end + core

            def to(k, slot=slot):
                return pltpu.make_async_remote_copy(
                    src_ref=ssq, dst_ref=ssq_ref.at[slot], send_sem=ssq_send.at[k], recv_sem=ssq_recv.at[slot],
                    device_id={"dp": (dp + k) % (2 * CHIPS)}, device_id_type=MESH,
                )

            local = pltpu.make_async_copy(ssq, ssq_ref.at[slot], io_sem.at[0])

            @pl.when(dp == holder)
            def _(to=to, local=local):
                local.start()
                for k in range(1, 2 * CHIPS):
                    to(k).start()
                local.wait()
                for k in range(1, 2 * CHIPS):
                    to(k).wait_send()

    for slot in range(4):
        holder = 2 * last * (slot // 2) + slot % 2

        @pl.when(dp != holder)
        def _(slot=slot):
            pltpu.make_async_remote_copy(
                src_ref=ssq, dst_ref=ssq_ref.at[slot], send_sem=ssq_send.at[0], recv_sem=ssq_recv.at[slot],
                device_id={"dp": dp}, device_id_type=MESH,
            ).wait_recv()

    for p in range(3):
        pair_copy(3 * (NS - 2) + p).wait_send()
        pair_copy(3 * (NS - 1) + p).wait_send()

    for way in ways:

        @pl.when(way.place < last)
        def _(way=way):
            repeat(SLOTS, lambda k: way.hop(UNITS - SLOTS + k).wait_send())

        def close(n, way=way):
            @pl.when(way.passes(n))
            def _():
                way.spread(n).wait_send()

            @pl.when(way.holds(n))
            def _():
                way.share(n).wait()

        repeat(UNITS, close)


def gradients(x, dy, w_gate, w_up, w_down):
    _, T, D = x.shape
    F = w_gate.shape[2]
    FS = F // PARTS
    RT, RD = min(512, T // 2), min(256, T)
    anywhere = pl.BlockSpec(memory_space=pl.ANY)
    dma = pltpu.SemaphoreType.DMA
    return pl.pallas_call(
        functools.partial(gradients_kernel, (T, D, FS, RT, RD)),
        out_shape=(
            jax.ShapeDtypeStruct((NS, 3, 4, D // 4, FS), BF16),
            jax.ShapeDtypeStruct((NS, 3, D // 2, FS), BF16),
            jax.ShapeDtypeStruct((NS, 3, D // 2, FS), BF16),
            jax.ShapeDtypeStruct((2, NS, 3, D // 4, FS), BF16),
            jax.ShapeDtypeStruct((4, 8, FS), F32),
            jax.ShapeDtypeStruct((T, D), BF16),
        ),
        in_specs=[anywhere] * 5,
        out_specs=(anywhere,) * 6,
        scratch_shapes=[
            pltpu.VMEM((T, D), BF16),
            pltpu.VMEM((D, T), BF16),
            pltpu.VMEM((T, D), BF16),
            pltpu.VMEM((D, T), BF16),
            pltpu.VMEM((T, D), F32),
            pltpu.VMEM((2, D, 2 * FS), BF16),
            pltpu.VMEM((2, FS, D), BF16),
            pltpu.VMEM((T, FS), BF16),
            pltpu.VMEM((T, 2 * FS), BF16),
            pltpu.VMEM((2, 3, D, FS), BF16),
            pltpu.VMEM((2, 3, D // 4, FS), BF16),
            pltpu.VMEM((2, SLOTS, D // 4, FS), BF16),
            pltpu.VMEM((8, FS), F32),
            dma((2, 3)),
            dma((3,)),
            dma((2, 3)),
            dma((2, 3)),
            dma((NS, 3)),
            dma((2, 3)),
            dma((2, SLOTS)),
            dma((2, NS, 3)),
            dma((SLOTS,)),
            dma((2, WHOLE + CHIPS, 3)),
            dma((2, WHOLE + CHIPS, 3)),
            dma((2, NS, 3)),
            dma((2, NS, 3)),
            dma((2 * CHIPS,)),
            dma((4,)),
        ],
        compiler_params=pltpu.CompilerParams(collective_id=0, has_side_effects=True, vmem_limit_bytes=66_000_000),
        name="gradients",
    )(x, dy, w_gate, w_up, w_down)


SUBS, DEEP = 4, 6


def adamw_kernel(count, work, n_in, aliased, *refs):
    refs = list(refs)

    def take(n):
        out, refs[:n] = refs[:n], []
        return out

    ssq_ref, g_ref = take(2)
    back = take(n_in)
    arrays = take(9)
    take(9 if aliased else 0)
    results = take(9)
    bufs, outs = take(9), take(9)
    gv, g_sem, in_sem, out_sem = take(4)
    quarter, FS = gv.shape[2:]
    few, part = quarter // SUBS, FS // SUBS
    dp = lax.axis_index("dp")
    z, c = dp // 2, dp % 2
    total = SUBS * len(work)
    alone = 4 * work[0][0] + work[0][1]
    rest = 4 * work[-1][0] + 4 - len(work)
    run = all(4 * i + b == alone + at for at, (i, b, _) in enumerate(work))

    def here(k, source):
        return pltpu.make_async_copy(source, gv.at[k], g_sem.at[k])

    def fetch(k):
        i, b, came = work[k]
        place = z if b < 2 else CHIPS - 1 - z
        for p in range(CHIPS):
            if came[p] is None:

                @pl.when(place == p)
                def _():
                    here(k, g_ref.at[i, :, b]).start()

            else:
                for core in range(2):

                    @pl.when((place == p) & (c == core))
                    def _(at=came[p][0 if core == b // 2 else 1]):
                        here(k, back[at].at[0, :, b % 2]).start()

    def blocks(n):
        k, sub = n // SUBS, n % SUBS
        at = alone + k if run else jnp.where(k == 0, alone, rest + k)
        i, b = at // 4, at % 4
        layer, hidden, q = 1 - i // PARTS, i % PARTS, b % 2 * 2 + b // 2
        across = (layer, pl.ds(pl.multiple_of(q * quarter + sub * few, few), few), pl.ds(pl.multiple_of(hidden * FS, FS), FS))
        down = (layer, pl.ds(pl.multiple_of(hidden * FS + sub * part, part), part), pl.ds(pl.multiple_of(q * quarter, quarter), quarter))
        return across, across, down

    def copies(n, inward):
        slot, where = n % DEEP, blocks(n)
        if inward:
            return [pltpu.make_async_copy(arrays[k].at[where[k % 3]], bufs[k].at[slot], in_sem.at[slot, k]) for k in range(9)]
        return [pltpu.make_async_copy(outs[k].at[slot], results[k].at[where[k % 3]], out_sem.at[slot, k]) for k in range(9)]

    def start(n, inward):
        for copy in copies(n, inward):
            copy.start()

    def wait(n, inward):
        for copy in copies(n, inward):
            copy.wait()

    fetch(0)
    for n in range(min(DEEP - 1, total)):
        start(n, True)
    for k in range(1, len(work)):
        fetch(k)
    factor = jnp.minimum(1.0, 0.5 * lax.rsqrt(jnp.sum(ssq_ref[...]) / count + 1e-30))

    def piece(n, _):
        k, sub, slot = n // SUBS, n % SUBS, n % DEEP

        @pl.when(sub == 0)
        def _():
            here(k, g_ref.at[0, :, 0]).wait()

        @pl.when(n + DEEP - 1 < total)
        def _():
            start(n + DEEP - 1, True)

        wait(n, True)

        @pl.when(n >= DEEP)
        def _():
            wait(n - DEEP, False)

        def update(number, g):
            g = g * factor
            m = 0.9 * bufs[3 + number][slot] + 0.1 * g
            v = 0.95 * bufs[6 + number][slot] + 0.05 * g * g
            w = bufs[number][slot].astype(F32)
            outs[number][slot] = (w - 0.02 * (m * lax.rsqrt(v + 1e-8) + 0.1 * w)).astype(BF16)
            outs[3 + number][slot] = m
            outs[6 + number][slot] = v

        rows = pl.ds(pl.multiple_of(sub * few, few), few)
        update(0, gv[k, 1, rows, :].astype(F32))
        update(1, gv[k, 2, rows, :].astype(F32))
        update(2, gv[k, 0, :, pl.ds(pl.multiple_of(sub * part, part), part)].astype(F32).T)
        start(n, False)
        return 0

    lax.fori_loop(0, total, piece, 0)
    lax.fori_loop(max(total - DEEP, 0), total, lambda n, _: (wait(n, False), 0)[1], 0)


def adamw(ssq, g, arrays, results, listed, back):
    _, _, _, quarter, FS = g.shape
    anywhere = pl.BlockSpec(memory_space=pl.ANY)
    size = 3 * len(listed) * quarter * FS
    ins = [ssq, g, *back, *arrays, *(results or ())]
    shapes = [(DEEP, quarter // SUBS, FS)] * 2 + [(DEEP, FS // SUBS, quarter)]
    bufs = [pltpu.VMEM(shapes[k % 3], a.dtype) for k, a in enumerate(arrays)]
    return pl.pallas_call(
        functools.partial(adamw_kernel, float(g.size), listed, len(back), bool(results)),
        in_specs=[pl.BlockSpec(memory_space=pltpu.VMEM)] + [anywhere] * (len(ins) - 1),
        out_specs=[anywhere] * 9,
        out_shape=[jax.ShapeDtypeStruct(a.shape, a.dtype) for a in arrays],
        input_output_aliases={len(ins) - 9 + k: k for k in range(9)} if results else {},
        scratch_shapes=[
            *bufs,
            *bufs,
            pltpu.VMEM((len(listed), 3, quarter, FS), BF16),
            pltpu.SemaphoreType.DMA((len(listed),)),
            pltpu.SemaphoreType.DMA((DEEP, 9)),
            pltpu.SemaphoreType.DMA((DEEP, 9)),
        ],
        compiler_params=pltpu.CompilerParams(vmem_limit_bytes=66_000_000),
        cost_estimate=pl.CostEstimate(flops=16 * size, bytes_accessed=22 * size, transcendentals=size),
        name="adamw",
    )(*ins)


def load_kernel(i, g_ref, _, sent_ref, buf, sem):
    dp = lax.axis_index("dp")
    z, c = dp // 2, dp % 2

    @pl.when(z == (CHIPS - 1) * (1 - c))
    def _():
        pieces = buf.shape[0]
        loads = [pltpu.make_async_copy(g_ref.at[i, p, pl.ds(2 * c, 2)], buf.at[p], sem.at[0, p]) for p in range(pieces)]
        stores = [pltpu.make_async_copy(buf.at[p], sent_ref.at[0, p], sem.at[1, p]) for p in range(pieces)]
        for load in loads:
            load.start()
        for load, store in zip(loads, stores, strict=True):
            load.wait()
            store.start()
        for store in stores:
            store.wait()


def load(g, i, came):
    anywhere = pl.BlockSpec(memory_space=pl.ANY)
    return pl.pallas_call(
        functools.partial(load_kernel, i),
        in_specs=[anywhere, anywhere],
        out_specs=anywhere,
        out_shape=jax.ShapeDtypeStruct(came.shape, came.dtype),
        input_output_aliases={1: 0},
        scratch_shapes=[pltpu.VMEM(came.shape[1:], BF16), pltpu.SemaphoreType.DMA((2, 3))],
        compiler_params=pltpu.CompilerParams(vmem_limit_bytes=66_000_000),
        cost_estimate=pl.CostEstimate(flops=came.size, bytes_accessed=4 * came.size, transcendentals=0),
        name="load",
    )(g, came)


def finish(g, ssq, arrays):
    _, _, _, quarter, FS = g.shape
    last = CHIPS - 1
    dp = lax.axis_index("dp")
    z, c = dp // 2, dp % 2
    place = jnp.where(c == 0, z, last - z)
    stages = NS - WHOLE
    ready = [(i, b, (None,) * CHIPS) for i in range(WHOLE) for b in range(4)]
    first = min(5, 2 * WHOLE)
    extra = 4 * WHOLE - 2 * first
    back, index, results = [], {}, None

    def units(u):
        came = tuple(index[u - p] if p < last and u >= p else None for p in range(CHIPS))
        return [(WHOLE + u, b, came) for b in range(4)]

    def update(results, listed):
        used = sorted({at for _, _, came in listed for pair in came if pair for at in pair})
        where = {at: k for k, at in enumerate(used)}
        listed = [(i, b, tuple(pair and tuple(where[at] for at in pair) for pair in came)) for i, b, came in listed]
        return adamw(ssq, g, arrays, results, listed, [back[at] for at in used])

    def device(place, core):
        return 2 * (place if core == 0 else last - place) + core

    sent = lax.dynamic_slice(g, (WHOLE + place - 1, jnp.int32(0), 2 * c, jnp.int32(0), jnp.int32(0)), (1, 3, 2, quarter, FS))
    pending = None
    for s in range(stages + 2):
        if s < stages:
            moves = [(device(p, core), device(p - 1, core)) for p in range(1, CHIPS) if s + p - 1 < stages for core in range(2)]
            newest = lax.ppermute(sent, "dp", moves)
        if pending is not None:
            back.append(lax.ppermute(*pending))
            pending = None
        many = first if s < 2 else 1 if s - 2 < extra else 0
        listed, ready = ready[:many], ready[many:]
        if s >= 2:
            listed = listed + units(s - 2)
        results = update(results, listed)
        if s < stages:
            sent = load(g, WHOLE + s + last, newest) if s + last < stages else newest
            index[s] = (len(back), len(back) + 1)
            back.append(sent)
            pending = (sent, "dp", [(to, to + 1 - 2 * (to % 2)) for _, to in moves])
    return results


def solution(mesh):
    def step(x, dy, *arrays):
        g, *_, ssq, _ = gradients(x, dy, *arrays[:3])
        return tuple(finish(g, ssq, arrays))

    return jax.shard_map(
        step,
        mesh=mesh,
        in_specs=(P(("rep", "dp"), None, None),) * 2 + (P(None, None, None),) * 9,
        out_specs=(P("rep", None, None),) * 9,
        check_vma=False,
    )
```

```python
import functools

import jax
import jax.numpy as jnp
from jax import lax
from jax.experimental import pallas as pl
from jax.experimental.pallas import tpu as pltpu
from jax.sharding import PartitionSpec as P


MESH = pl.DeviceIdType.MESH
CHIPS = 4
PARTS = 8
NS = 2 * PARTS
KEPT = PARTS - 2
WHOLE = 6
LAG = 3
SLOTS = 4
F32, BF16 = jnp.float32, jnp.bfloat16


def dot(a, b):
    return jnp.dot(a, b, preferred_element_type=F32)


def dot_nt(a, b):
    return lax.dot_general(a, b, (((1,), (1,)), ((), ())), preferred_element_type=F32)


def inverse_size(wide):
    return lax.rsqrt(jnp.mean(wide * wide, -1, keepdims=True) + 1e-6)


def gradients_kernel(
    sizes,
    x_ref, dy_ref, wg_ref, wu_ref, wd_ref,
    g_ref, own_ref, pair_ref, chain_ref, ssq_ref, h_ref, dgu_ref,
    a, at, up, upt, acc, wgu, wd, hid, dgu, gb, st, out, ssq,
    w_sem, io_sem, dgu_sem, pair_send, own_sem, pair_recv, ld_sem, chain_send, chain_recv, keep_sem, pass_send, pass_recv, mate_send, mate_recv, ssq_send, ssq_recv,
):
    T, D, FS, RT, RD = sizes
    UNITS = 3 * NS
    half, quarter = D // 2, D // 4
    dp = lax.axis_index("dp")
    z, c = dp // 2, dp % 2
    mate = dp + 1 - 2 * c
    last = CHIPS - 1

    barrier = pltpu.get_barrier_semaphore()
    for k in range(1, 2 * CHIPS):
        pl.semaphore_signal(barrier, inc=1, device_id={"dp": (dp + k) % (2 * CHIPS)}, device_id_type=MESH)

    def weight_copies(w):
        phase = w // PARTS
        layer = jnp.where((phase == 1) | (phase == 2), 1, 0)
        part = jnp.where(phase == 2, w + KEPT, w) % PARTS
        columns = pl.ds(pl.multiple_of(part * FS, FS), FS)
        slot = w % 2
        both = (
            pltpu.make_async_copy(wg_ref.at[layer, :, columns], wgu.at[slot, :, pl.ds(0, FS)], w_sem.at[slot, 0]),
            pltpu.make_async_copy(wu_ref.at[layer, :, columns], wgu.at[slot, :, pl.ds(FS, FS)], w_sem.at[slot, 1]),
        )
        return both, pltpu.make_async_copy(wd_ref.at[layer, columns, :], wd.at[slot], w_sem.at[slot, 2]), phase != 2

    def fetch(w):
        both, down, needed = weight_copies(w)
        for copy in both:
            copy.start()

        @pl.when(needed)
        def _():
            down.start()

    def fetched(w):
        both, down, needed = weight_copies(w)
        for copy in both:
            copy.wait()

        @pl.when(needed)
        def _():
            down.wait()

    def rows_of(r, size):
        return pl.ds(pl.multiple_of(r * size, size), size)

    def repeat(n, body):
        lax.fori_loop(0, n, lambda r, _: (body(r), 0)[1], 0)

    def over_rows(total, size, body):
        repeat(total // size, lambda r: body(rows_of(r, size)))

    load_x = pltpu.make_async_copy(x_ref.at[0], a, io_sem.at[0])
    load_x.start()
    fetch(0)
    load_again = pltpu.make_async_copy(x_ref.at[0], dgu.at[0], io_sem.at[1])
    load_again.start()
    load_dy = pltpu.make_async_copy(dy_ref.at[0], up, io_sem.at[2])
    load_dy.start()
    ssq[...] = jnp.zeros_like(ssq)
    load_x.wait()

    def norm_in_place(rows):
        wide = a[rows, :].astype(F32)
        a[rows, :] = (wide * inverse_size(wide)).astype(BF16)

    over_rows(T, RD, norm_in_place)

    def forward(j):
        slot = j % 2
        fetched(j)
        fetch(j + 1)

        def tile(rows):
            gu = dot(a[rows, :], wgu[slot])
            gate, lift = gu[:, :FS], gu[:, FS:]
            hidden = (gate * jax.nn.sigmoid(gate) * lift).astype(BF16)
            acc[rows, :] = jnp.where(j > 0, acc[rows, :], 0.0) + dot(hidden, wd[slot])

        over_rows(T, RT, tile)

    repeat(PARTS, forward)

    load_again.wait()

    def close_forward(rows):
        h = dgu[0, rows, :].astype(F32) + acc[rows, :].astype(BF16).astype(F32)
        h = h.astype(BF16)
        dgu[0, rows, :] = h
        wide = h.astype(F32)
        a[rows, :] = (wide * inverse_size(wide)).astype(BF16)

    over_rows(T, RD, close_forward)
    save_h = pltpu.make_async_copy(dgu.at[0], h_ref, io_sem.at[0])
    save_h.start()

    def turn(source, target):
        def tile(rows):
            target[:, rows] = source[rows, :].T

        over_rows(T, RD, tile)

    load_dy.wait()
    turn(a, at)
    turn(up, upt)
    save_h.wait()
    pl.semaphore_wait(barrier, 2 * CHIPS - 1)

    reload_x = pltpu.make_async_copy(x_ref.at[0], a, io_sem.at[1])

    load_h = pltpu.make_async_copy(h_ref, dgu.at[0], io_sem.at[0])

    def cross_layers():
        reload_x.wait()
        over_rows(T, RD, norm_in_place)
        turn(a, at)
        load_h.wait()

        def tile(rows):
            wide = dgu[0, rows, :].astype(F32)
            scale = inverse_size(wide)
            da = acc[rows, :].astype(BF16).astype(F32)
            along = jnp.sum(da * wide, -1, keepdims=True) * (1.0 / D)
            dh = (scale * da - wide * (scale * scale * scale * along)).astype(BF16)
            up[rows, :] = (up[rows, :].astype(F32) + dh.astype(F32)).astype(BF16)

        over_rows(T, RD, tile)
        turn(up, upt)

    def half_of(core):
        return pl.ds(pl.multiple_of(core * half, half), half)

    def pair_copy(n):
        i, p = n // 3, n % 3
        return pltpu.make_async_remote_copy(
            src_ref=gb.at[i % 2, p, half_of(1 - c), :], dst_ref=pair_ref.at[i, p], send_sem=pair_send.at[i % 2, p], recv_sem=pair_recv.at[i, p],
            device_id={"dp": mate}, device_id_type=MESH,
        )

    def own_copy(n):
        i, p = n // 3, n % 3
        return pltpu.make_async_copy(gb.at[i % 2, p, half_of(c), :], own_ref.at[i, p], own_sem.at[i % 2, p])

    class Way:
        def __init__(self, d):
            self.d = d
            self.place = z if d == 0 else last - z
            self.step = 2 if d == 0 else -2
            self.small = pl.ds(d * quarter, quarter)
            self.block = 2 * d + c

        def loads(self, n):
            d, i, p = self.d, n // 3, n % 3
            return (
                pltpu.make_async_copy(own_ref.at[i, p, self.small, :], st.at[d, 0], ld_sem.at[d, 0]),
                pltpu.make_async_copy(pair_ref.at[i, p, self.small, :], st.at[d, 1], ld_sem.at[d, 1]),
                pltpu.make_async_copy(chain_ref.at[d, i, p], st.at[d, 2], ld_sem.at[d, 2]),
            )

        def hop(self, n):
            d, i, p = self.d, n // 3, n % 3
            return pltpu.make_async_remote_copy(
                src_ref=out.at[d, n % SLOTS], dst_ref=chain_ref.at[d, i, p], send_sem=chain_send.at[d, n % SLOTS], recv_sem=chain_recv.at[d, i, p],
                device_id={"dp": (dp + self.step) % (2 * CHIPS)}, device_id_type=MESH,
            )

        def keep(self, n):
            return pltpu.make_async_copy(out.at[self.d, n % SLOTS], g_ref.at[n // 3, n % 3, self.block], keep_sem.at[n % SLOTS])

        def spread(self, n):
            d, i, p = self.d, n // 3, n % 3
            return pltpu.make_async_remote_copy(
                src_ref=g_ref.at[i, p, self.block], dst_ref=g_ref.at[i, p, self.block], send_sem=pass_send.at[d, i, p], recv_sem=pass_recv.at[d, i, p],
                device_id={"dp": (dp - self.step + 2 * CHIPS) % (2 * CHIPS)}, device_id_type=MESH,
            )

        def share(self, n):
            d, i, p = self.d, n // 3, n % 3
            return pltpu.make_async_remote_copy(
                src_ref=g_ref.at[i, p, self.block], dst_ref=g_ref.at[i, p, self.block], send_sem=mate_send.at[d, i, p], recv_sem=mate_recv.at[d, i, p],
                device_id={"dp": mate}, device_id_type=MESH,
            )

        def reaches(self, n, place):
            return last - place <= WHOLE + last - 1 - n // 3

        def holds(self, n):
            return (self.place == last) | self.reaches(n, self.place)

        def passes(self, n):
            return (self.place > 0) & self.reaches(n, self.place - 1)

    ways = (Way(0), Way(1))

    def inside(n):
        return (n >= 0) & (n < UNITS)

    def unit(k):
        return jnp.where(k < 3 * PARTS, k, jnp.where(k < 3 * PARTS + PARTS, -1, k - PARTS))

    def start_tick(k):
        newest = unit(k - 2)

        @pl.when(inside(newest))
        def _():
            own_copy(newest).wait()
            pair_copy(newest).wait_recv()

        for way in ways:
            n = unit(k - 2 - LAG * way.place)

            @pl.when(inside(n))
            def _(way=way, n=n):
                own, pair, chain = way.loads(n)
                own.start()
                pair.start()

                @pl.when(way.place > 0)
                def _():
                    way.hop(n).wait_recv()
                    chain.start()

    def finish_tick(k):
        for way in ways:
            d = way.d
            n = unit(k - 2 - LAG * way.place)

            @pl.when(inside(n))
            def _(way=way, d=d, n=n):
                own, pair, chain = way.loads(n)
                own.wait()
                pair.wait()

                @pl.when((way.place < last) & (n >= SLOTS))
                def _():
                    way.hop(n - SLOTS).wait_send()

                def add(so_far):
                    wide = st[d, 0].astype(F32) + st[d, 1].astype(F32)
                    if so_far:
                        wide += st[d, 2].astype(F32)
                    rounded = wide.astype(BF16)
                    out[d, n % SLOTS] = rounded
                    return rounded.astype(F32)

                @pl.when(way.place == 0)
                def _():
                    add(False)
                    way.hop(n).start()

                @pl.when((way.place > 0) & (way.place < last))
                def _():
                    chain.wait()
                    add(True)
                    way.hop(n).start()

                @pl.when(way.place == last)
                def _():
                    chain.wait()
                    total = add(True)
                    way.keep(n).start()
                    ssq[...] += jnp.sum((total * total).reshape(quarter // 8, 8, FS), 0)

        for way in ways:
            n = unit(k - 3 - LAG * (2 * last - way.place))

            @pl.when(inside(n))
            def _(way=way, n=n):
                @pl.when(way.place == last)
                def _():
                    way.keep(n).wait()

                @pl.when((way.place < last) & way.holds(n))
                def _():
                    way.spread(n).wait_recv()

                @pl.when(way.passes(n))
                def _():
                    way.spread(n).start()

                @pl.when(way.holds(n))
                def _():
                    way.share(n).start()

    def dgu_copy(t):
        return pltpu.make_async_copy(dgu.at[t % 2], dgu_ref.at[t], dgu_sem.at[t % 2])

    def backward(t, tick, w, early):
        slot, half_slot = w % 2, t % 2
        fetched(w)

        @pl.when(w < 4 * PARTS - 1)
        def _():
            fetch(w + 1)

        if early:

            @pl.when((t >= 2) & (t < PARTS))
            def _():
                dgu_copy(t - 2).wait()

        def hidden_half(k):
            start_tick(tick + k)

            def tile(r):
                rows = rows_of(k * (T // RT // 2) + r, RT)
                gu = dot(a[rows, :], wgu[slot])
                dh = dot_nt(up[rows, :], wd[slot]).astype(BF16).astype(F32)
                gate, lift = gu[:, :FS], gu[:, FS:]
                s = jax.nn.sigmoid(gate)
                silu = gate * s
                hid[rows, :] = (silu * lift).astype(BF16)
                dgu[half_slot, rows, :FS] = (dh * lift * (s + silu * (1.0 - s))).astype(BF16)
                dgu[half_slot, rows, FS:] = (dh * silu).astype(BF16)

            repeat(T // RT // 2, tile)
            finish_tick(tick + k)

        repeat(2, hidden_half)

        if early:

            @pl.when(t < KEPT)
            def _():
                dgu_copy(t).start()

        @pl.when(t >= 2)
        def _():
            for p in range(3):
                pair_copy(3 * (t - 2) + p).wait_send()

        def down_half(k):
            rows = half_of(jnp.where(k == 0, 1 - c, c))
            gb[half_slot, 0, rows, :] = dot(upt[rows, :], hid[...]).astype(BF16)

            @pl.when(k == 0)
            def _():
                pair_copy(3 * t).start()

            @pl.when(k == 1)
            def _():
                own_copy(3 * t).start()

        repeat(2, down_half)

        def both_half(k):
            @pl.when(k == 1)
            def _():
                start_tick(tick + 2)

            rows = half_of(jnp.where(k == 0, 1 - c, c))
            both = dot(at[rows, :], dgu[half_slot]).astype(BF16)
            gb[half_slot, 1, rows, :] = both[:, :FS]
            gb[half_slot, 2, rows, :] = both[:, FS:]

            @pl.when(k == 0)
            def _():
                pair_copy(3 * t + 1).start()
                pair_copy(3 * t + 2).start()

            @pl.when(k == 1)
            def _():
                own_copy(3 * t + 1).start()
                own_copy(3 * t + 2).start()
                finish_tick(tick + 2)

        repeat(2, both_half)

    def dgu_load(s):
        return pltpu.make_async_copy(dgu_ref.at[s + KEPT - PARTS], dgu.at[s % 2], dgu_sem.at[s % 2])

    def sum_for_a(s):
        w = 2 * PARTS + s
        fetched(w)
        fetch(w + 1)

        @pl.when(s >= PARTS - KEPT)
        def _():
            dgu_load(s).wait()

        @pl.when((s >= 1) & (s < PARTS - 1))
        def _():
            dgu_load(s + 1).start()

        @pl.when(s == PARTS - 1)
        def _():
            load_h.start()

        start_tick(3 * PARTS + s)

        def tile(rows):
            acc[rows, :] = jnp.where(s > 0, acc[rows, :], 0.0) + dot_nt(dgu[s % 2, rows, :], wgu[w % 2])

        over_rows(T, RT, tile)
        finish_tick(3 * PARTS + s)

    def slice_of(i):
        @pl.when(i == PARTS)
        def _():
            reload_x.start()
            repeat(PARTS, sum_for_a)
            cross_layers()

        later = i >= PARTS
        backward(i, jnp.where(later, 3 * i + PARTS, 3 * i), jnp.where(later, i + 2 * PARTS, i + PARTS), True)

    repeat(NS, slice_of)

    def drain(k):
        start_tick(UNITS + PARTS + k)
        finish_tick(UNITS + PARTS + k)

    ticks = max(UNITS + 2 + LAG * last + 1, 3 * (WHOLE + last - 1) + 2 + LAG * 2 * last + 1)
    repeat(ticks - UNITS, drain)

    for at_end in range(2):
        for core in range(2):
            slot = 2 * at_end + core
            holder = 2 * last * at_end + core

            def to(k, slot=slot):
                return pltpu.make_async_remote_copy(
                    src_ref=ssq, dst_ref=ssq_ref.at[slot], send_sem=ssq_send.at[k], recv_sem=ssq_recv.at[slot],
                    device_id={"dp": (dp + k) % (2 * CHIPS)}, device_id_type=MESH,
                )

            local = pltpu.make_async_copy(ssq, ssq_ref.at[slot], io_sem.at[0])

            @pl.when(dp == holder)
            def _(to=to, local=local):
                local.start()
                for k in range(1, 2 * CHIPS):
                    to(k).start()
                local.wait()
                for k in range(1, 2 * CHIPS):
                    to(k).wait_send()

    for slot in range(4):
        holder = 2 * last * (slot // 2) + slot % 2

        @pl.when(dp != holder)
        def _(slot=slot):
            pltpu.make_async_remote_copy(
                src_ref=ssq, dst_ref=ssq_ref.at[slot], send_sem=ssq_send.at[0], recv_sem=ssq_recv.at[slot],
                device_id={"dp": dp}, device_id_type=MESH,
            ).wait_recv()

    for p in range(3):
        pair_copy(3 * (NS - 2) + p).wait_send()
        pair_copy(3 * (NS - 1) + p).wait_send()

    for way in ways:

        @pl.when(way.place < last)
        def _(way=way):
            repeat(SLOTS, lambda k: way.hop(UNITS - SLOTS + k).wait_send())

        def close(n, way=way):
            @pl.when(way.passes(n))
            def _():
                way.spread(n).wait_send()

            @pl.when(way.holds(n))
            def _():
                way.share(n).wait()

        repeat(UNITS, close)


def gradients(x, dy, w_gate, w_up, w_down):
    _, T, D = x.shape
    F = w_gate.shape[2]
    FS = F // PARTS
    RT, RD = min(512, T // 2), min(256, T)
    anywhere = pl.BlockSpec(memory_space=pl.ANY)
    dma = pltpu.SemaphoreType.DMA
    return pl.pallas_call(
        functools.partial(gradients_kernel, (T, D, FS, RT, RD)),
        out_shape=(
            jax.ShapeDtypeStruct((NS, 3, 4, D // 4, FS), BF16),
            jax.ShapeDtypeStruct((NS, 3, D // 2, FS), BF16),
            jax.ShapeDtypeStruct((NS, 3, D // 2, FS), BF16),
            jax.ShapeDtypeStruct((2, NS, 3, D // 4, FS), BF16),
            jax.ShapeDtypeStruct((4, 8, FS), F32),
            jax.ShapeDtypeStruct((T, D), BF16),
            jax.ShapeDtypeStruct((KEPT, T, 2 * FS), BF16),
        ),
        in_specs=[anywhere] * 5,
        out_specs=(anywhere,) * 7,
        scratch_shapes=[
            pltpu.VMEM((T, D), BF16),
            pltpu.VMEM((D, T), BF16),
            pltpu.VMEM((T, D), BF16),
            pltpu.VMEM((D, T), BF16),
            pltpu.VMEM((T, D), F32),
            pltpu.VMEM((2, D, 2 * FS), BF16),
            pltpu.VMEM((2, FS, D), BF16),
            pltpu.VMEM((T, FS), BF16),
            pltpu.VMEM((2, T, 2 * FS), BF16),
            pltpu.VMEM((2, 3, D, FS), BF16),
            pltpu.VMEM((2, 3, D // 4, FS), BF16),
            pltpu.VMEM((2, SLOTS, D // 4, FS), BF16),
            pltpu.VMEM((8, FS), F32),
            dma((2, 3)),
            dma((3,)),
            dma((2,)),
            dma((2, 3)),
            dma((2, 3)),
            dma((NS, 3)),
            dma((2, 3)),
            dma((2, SLOTS)),
            dma((2, NS, 3)),
            dma((SLOTS,)),
            dma((2, WHOLE + CHIPS, 3)),
            dma((2, WHOLE + CHIPS, 3)),
            dma((2, NS, 3)),
            dma((2, NS, 3)),
            dma((2 * CHIPS,)),
            dma((4,)),
        ],
        compiler_params=pltpu.CompilerParams(collective_id=0, has_side_effects=True, vmem_limit_bytes=66_000_000),
        name="gradients",
    )(x, dy, w_gate, w_up, w_down)


SUBS, DEEP = 2, 4


def adamw_kernel(count, work, n_in, aliased, *refs):
    refs = list(refs)

    def take(n):
        out, refs[:n] = refs[:n], []
        return out

    ssq_ref, g_ref = take(2)
    back = take(n_in)
    arrays = take(9)
    take(9 if aliased else 0)
    results = take(9)
    bufs, outs = take(9), take(9)
    gv, g_sem, in_sem, out_sem = take(4)
    quarter, FS = gv.shape[2:]
    few, part = quarter // SUBS, FS // SUBS
    dp = lax.axis_index("dp")
    z, c = dp // 2, dp % 2
    total = SUBS * len(work)
    numbers = [4 * i + b for i, b, _ in work]
    cut = next((k for k in range(1, len(work)) if numbers[k] != numbers[k - 1] + 1), len(work))

    def here(k, source):
        return pltpu.make_async_copy(source, gv.at[k], g_sem.at[k])

    def fetch(k):
        i, b, came = work[k]
        place = z if b < 2 else CHIPS - 1 - z
        for p in range(CHIPS):
            if came[p] is None:

                @pl.when(place == p)
                def _():
                    here(k, g_ref.at[i, :, b]).start()

            else:
                for core in range(2):

                    @pl.when((place == p) & (c == core))
                    def _(at=came[p][0 if core == b // 2 else 1]):
                        here(k, back[at].at[0, :, b % 2]).start()

    def blocks(n):
        k, sub = n // SUBS, n % SUBS
        at = numbers[0] + k if cut == len(work) else jnp.where(k < cut, numbers[0] + k, numbers[cut] - cut + k)
        i, b = at // 4, at % 4
        layer, hidden, q = 1 - i // PARTS, i % PARTS, b % 2 * 2 + b // 2
        across = (layer, pl.ds(pl.multiple_of(q * quarter + sub * few, few), few), pl.ds(pl.multiple_of(hidden * FS, FS), FS))
        down = (layer, pl.ds(pl.multiple_of(hidden * FS + sub * part, part), part), pl.ds(pl.multiple_of(q * quarter, quarter), quarter))
        return across, across, down

    def copies(n, inward):
        slot, where = n % DEEP, blocks(n)
        if inward:
            return [pltpu.make_async_copy(arrays[k].at[where[k % 3]], bufs[k].at[slot], in_sem.at[slot, k]) for k in range(9)]
        return [pltpu.make_async_copy(outs[k].at[slot], results[k].at[where[k % 3]], out_sem.at[slot, k]) for k in range(9)]

    def start(n, inward):
        for copy in copies(n, inward):
            copy.start()

    def wait(n, inward):
        for copy in copies(n, inward):
            copy.wait()

    fetch(0)
    for n in range(min(DEEP - 1, total)):
        start(n, True)
    for k in range(1, len(work)):
        fetch(k)
    factor = jnp.minimum(1.0, 0.5 * lax.rsqrt(jnp.sum(ssq_ref[...]) / count + 1e-30))

    def piece(n, _):
        k, sub, slot = n // SUBS, n % SUBS, n % DEEP

        @pl.when(sub == 0)
        def _():
            here(k, g_ref.at[0, :, 0]).wait()

        @pl.when(n + DEEP - 1 < total)
        def _():
            start(n + DEEP - 1, True)

        wait(n, True)

        @pl.when(n >= DEEP)
        def _():
            wait(n - DEEP, False)

        def update(number, g):
            g = g * factor
            m = 0.9 * bufs[3 + number][slot] + 0.1 * g
            v = 0.95 * bufs[6 + number][slot] + 0.05 * g * g
            w = bufs[number][slot].astype(F32)
            outs[number][slot] = (w - 0.02 * (m * lax.rsqrt(v + 1e-8) + 0.1 * w)).astype(BF16)
            outs[3 + number][slot] = m
            outs[6 + number][slot] = v

        rows = pl.ds(pl.multiple_of(sub * few, few), few)
        update(0, gv[k, 1, rows, :].astype(F32))
        update(1, gv[k, 2, rows, :].astype(F32))
        update(2, gv[k, 0, :, pl.ds(pl.multiple_of(sub * part, part), part)].astype(F32).T)
        start(n, False)
        return 0

    lax.fori_loop(0, total, piece, 0)
    lax.fori_loop(max(total - DEEP, 0), total, lambda n, _: (wait(n, False), 0)[1], 0)


def adamw(ssq, g, arrays, results, listed, back):
    _, _, _, quarter, FS = g.shape
    anywhere = pl.BlockSpec(memory_space=pl.ANY)
    size = 3 * len(listed) * quarter * FS
    ins = [ssq, g, *back, *arrays, *(results or ())]
    shapes = [(DEEP, quarter // SUBS, FS)] * 2 + [(DEEP, FS // SUBS, quarter)]
    bufs = [pltpu.VMEM(shapes[k % 3], a.dtype) for k, a in enumerate(arrays)]
    return pl.pallas_call(
        functools.partial(adamw_kernel, float(g.size), listed, len(back), bool(results)),
        in_specs=[pl.BlockSpec(memory_space=pltpu.VMEM)] + [anywhere] * (len(ins) - 1),
        out_specs=[anywhere] * 9,
        out_shape=[jax.ShapeDtypeStruct(a.shape, a.dtype) for a in arrays],
        input_output_aliases={len(ins) - 9 + k: k for k in range(9)} if results else {},
        scratch_shapes=[
            *bufs,
            *bufs,
            pltpu.VMEM((len(listed), 3, quarter, FS), BF16),
            pltpu.SemaphoreType.DMA((len(listed),)),
            pltpu.SemaphoreType.DMA((DEEP, 9)),
            pltpu.SemaphoreType.DMA((DEEP, 9)),
        ],
        compiler_params=pltpu.CompilerParams(vmem_limit_bytes=66_000_000),
        cost_estimate=pl.CostEstimate(flops=16 * size, bytes_accessed=22 * size, transcendentals=size),
        name="adamw",
    )(*ins)


def load_kernel(i, g_ref, _, sent_ref, buf, sem):
    dp = lax.axis_index("dp")
    z, c = dp // 2, dp % 2

    @pl.when(z == (CHIPS - 1) * (1 - c))
    def _():
        pieces = buf.shape[0]
        loads = [pltpu.make_async_copy(g_ref.at[i, p, pl.ds(2 * c, 2)], buf.at[p], sem.at[0, p]) for p in range(pieces)]
        stores = [pltpu.make_async_copy(buf.at[p], sent_ref.at[0, p], sem.at[1, p]) for p in range(pieces)]
        for load in loads:
            load.start()
        for load, store in zip(loads, stores, strict=True):
            load.wait()
            store.start()
        for store in stores:
            store.wait()


def load(g, i, came):
    anywhere = pl.BlockSpec(memory_space=pl.ANY)
    return pl.pallas_call(
        functools.partial(load_kernel, i),
        in_specs=[anywhere, anywhere],
        out_specs=anywhere,
        out_shape=jax.ShapeDtypeStruct(came.shape, came.dtype),
        input_output_aliases={1: 0},
        scratch_shapes=[pltpu.VMEM(came.shape[1:], BF16), pltpu.SemaphoreType.DMA((2, 3))],
        compiler_params=pltpu.CompilerParams(vmem_limit_bytes=66_000_000),
        cost_estimate=pl.CostEstimate(flops=came.size, bytes_accessed=4 * came.size, transcendentals=0),
        name="load",
    )(g, came)


def finish(g, ssq, arrays):
    _, _, _, quarter, FS = g.shape
    last = CHIPS - 1
    dp = lax.axis_index("dp")
    z, c = dp // 2, dp % 2
    place = jnp.where(c == 0, z, last - z)
    stages = NS - WHOLE
    ready = [(i, b, (None,) * CHIPS) for i in range(WHOLE) for b in range(4)]
    first = min(6, 2 * WHOLE)
    spare = 4 * WHOLE - 2 * first
    more = [spare // (stages - 2) + (s < spare % (stages - 2)) for s in range(stages - 2)] + [0] * 2
    back, index, results = [], {}, None

    def units(u):
        came = tuple(index[u - p] if p < last and u >= p else None for p in range(CHIPS))
        return [(WHOLE + u, b, came) for b in range(4)]

    def update(results, listed):
        used = sorted({at for _, _, came in listed for pair in came if pair for at in pair})
        where = {at: k for k, at in enumerate(used)}
        listed = [(i, b, tuple(pair and tuple(where[at] for at in pair) for pair in came)) for i, b, came in listed]
        return adamw(ssq, g, arrays, results, listed, [back[at] for at in used])

    def device(place, core):
        return 2 * (place if core == 0 else last - place) + core

    sent = lax.dynamic_slice(g, (WHOLE + place - 1, jnp.int32(0), 2 * c, jnp.int32(0), jnp.int32(0)), (1, 3, 2, quarter, FS))
    pending = None
    for s in range(stages + 2):
        if s < stages:
            moves = [(device(p, core), device(p - 1, core)) for p in range(1, CHIPS) if s + p - 1 < stages for core in range(2)]
            newest = lax.ppermute(sent, "dp", moves)
        if pending is not None:
            back.append(lax.ppermute(*pending))
            pending = None
        many = first if s < 2 else more[s - 2]
        listed, ready = ready[:many], ready[many:]
        if s >= 2:
            listed = listed + units(s - 2)
        results = update(results, listed)
        if s < stages:
            sent = load(g, WHOLE + s + last, newest) if s + last < stages else newest
            index[s] = (len(back), len(back) + 1)
            back.append(sent)
            pending = (sent, "dp", [(to, to + 1 - 2 * (to % 2)) for _, to in moves])
    return results


def solution(mesh):
    def step(x, dy, *arrays):
        g, *_, ssq, _, _ = gradients(x, dy, *arrays[:3])
        return tuple(finish(g, ssq, arrays))

    return jax.shard_map(
        step,
        mesh=mesh,
        in_specs=(P(("rep", "dp"), None, None),) * 2 + (P(None, None, None),) * 9,
        out_specs=(P("rep", None, None),) * 9,
        check_vma=False,
    )
```

```python
import functools

import jax
import jax.numpy as jnp
from jax import lax
from jax.experimental import pallas as pl
from jax.experimental.pallas import tpu as pltpu
from jax.sharding import PartitionSpec as P


MESH = pl.DeviceIdType.MESH
CHIPS = 4
PARTS = 8
NS = 2 * PARTS
KEPT = PARTS - 2
WHOLE = 6
LAG = 3
SLOTS = 4
FOLD = 128
F32, BF16 = jnp.float32, jnp.bfloat16


def dot(a, b):
    return jnp.dot(a, b, preferred_element_type=F32)


def dot_nt(a, b):
    return lax.dot_general(a, b, (((1,), (1,)), ((), ())), preferred_element_type=F32)


def inverse_size(wide):
    return lax.rsqrt(jnp.mean(wide * wide, -1, keepdims=True) + 1e-6)


def gradients_kernel(
    sizes,
    x_ref, dy_ref, wg_ref, wu_ref, wd_ref,
    g_ref, own_ref, pair_ref, chain_ref, ssq_ref, sent_ref, h_ref, dgu_ref,
    a, at, up, upt, acc, wgu, wd, hid, dgu, gb, st, out, ssq, folded,
    w_sem, io_sem, dgu_sem, pair_send, own_sem, pair_recv, ld_sem, chain_send, chain_recv, keep_sem, pass_send, pass_recv, mate_send, mate_recv, ssq_send, ssq_recv,
):
    T, D, FS, RF, RT, RD = sizes
    UNITS = 3 * NS
    half, quarter = D // 2, D // 4
    dp = lax.axis_index("dp")
    z, c = dp // 2, dp % 2
    mate = dp + 1 - 2 * c
    last = CHIPS - 1

    barrier = pltpu.get_barrier_semaphore()
    for k in range(1, 2 * CHIPS):
        pl.semaphore_signal(barrier, inc=1, device_id={"dp": (dp + k) % (2 * CHIPS)}, device_id_type=MESH)

    def weight_copies(w):
        phase = w // PARTS
        layer = jnp.where((phase == 1) | (phase == 2), 1, 0)
        part = jnp.where(phase == 2, w + KEPT, w) % PARTS
        columns = pl.ds(pl.multiple_of(part * FS, FS), FS)
        slot = w % 2
        both = (
            pltpu.make_async_copy(wg_ref.at[layer, :, columns], wgu.at[slot, :, pl.ds(0, FS)], w_sem.at[slot, 0]),
            pltpu.make_async_copy(wu_ref.at[layer, :, columns], wgu.at[slot, :, pl.ds(FS, FS)], w_sem.at[slot, 1]),
        )
        return both, pltpu.make_async_copy(wd_ref.at[layer, columns, :], wd.at[slot], w_sem.at[slot, 2]), phase != 2

    def fetch(w):
        both, down, needed = weight_copies(w)
        for copy in both:
            copy.start()

        @pl.when(needed)
        def _():
            down.start()

    def fetched(w):
        both, down, needed = weight_copies(w)
        for copy in both:
            copy.wait()

        @pl.when(needed)
        def _():
            down.wait()

    def rows_of(r, size):
        return pl.ds(pl.multiple_of(r * size, size), size)

    def repeat(n, body):
        lax.fori_loop(0, n, lambda r, _: (body(r), 0)[1], 0)

    def over_rows(total, size, body):
        repeat(total // size, lambda r: body(rows_of(r, size)))

    load_x = pltpu.make_async_copy(x_ref.at[0], a, io_sem.at[0])
    load_x.start()
    fetch(0)
    load_again = pltpu.make_async_copy(x_ref.at[0], dgu.at[0], io_sem.at[1])
    load_again.start()
    load_dy = pltpu.make_async_copy(dy_ref.at[0], up, io_sem.at[2])
    load_dy.start()
    ssq[...] = jnp.zeros_like(ssq)
    load_x.wait()

    def norm_in_place(rows):
        wide = a[rows, :].astype(F32)
        a[rows, :] = (wide * inverse_size(wide)).astype(BF16)

    over_rows(T, RD, norm_in_place)

    def forward(j):
        slot = j % 2
        fetched(j)
        fetch(j + 1)

        def tile(rows):
            gu = dot(a[rows, :], wgu[slot])
            gate, lift = gu[:, :FS], gu[:, FS:]
            hidden = (gate * jax.nn.sigmoid(gate) * lift).astype(BF16)
            acc[rows, :] = jnp.where(j > 0, acc[rows, :], 0.0) + dot(hidden, wd[slot])

        over_rows(T, RF, tile)

    repeat(PARTS, forward)

    load_again.wait()
    load_dy.wait()

    def close_forward(rows):
        h = dgu[0, rows, :].astype(F32) + acc[rows, :].astype(BF16).astype(F32)
        h = h.astype(BF16)
        dgu[0, rows, :] = h
        wide = h.astype(F32)
        normed = (wide * inverse_size(wide)).astype(BF16)
        a[rows, :] = normed
        at[:, rows] = normed.T
        upt[:, rows] = up[rows, :].T

    over_rows(T, RD, close_forward)
    save_h = pltpu.make_async_copy(dgu.at[0], h_ref, io_sem.at[0])
    save_h.start()
    pl.semaphore_wait(barrier, 2 * CHIPS - 1)
    save_h.wait()

    reload_x = pltpu.make_async_copy(x_ref.at[0], a, io_sem.at[1])
    load_h = pltpu.make_async_copy(h_ref, dgu.at[0], io_sem.at[0])

    def cross_layers():
        reload_x.wait()
        load_h.wait()

        def tile(rows):
            wide = a[rows, :].astype(F32)
            normed = (wide * inverse_size(wide)).astype(BF16)
            a[rows, :] = normed
            at[:, rows] = normed.T
            wide = dgu[0, rows, :].astype(F32)
            scale = inverse_size(wide)
            da = acc[rows, :].astype(BF16).astype(F32)
            along = jnp.sum(da * wide, -1, keepdims=True) * (1.0 / D)
            dh = (scale * da - wide * (scale * scale * scale * along)).astype(BF16)
            new = (up[rows, :].astype(F32) + dh.astype(F32)).astype(BF16)
            up[rows, :] = new
            upt[:, rows] = new.T

        over_rows(T, RD, tile)

    def half_of(core):
        return pl.ds(pl.multiple_of(core * half, half), half)

    def pair_copy(n):
        i, p = n // 3, n % 3
        return pltpu.make_async_remote_copy(
            src_ref=gb.at[i % 2, p, half_of(1 - c), :], dst_ref=pair_ref.at[i, p], send_sem=pair_send.at[i % 2, p], recv_sem=pair_recv.at[i, p],
            device_id={"dp": mate}, device_id_type=MESH,
        )

    def own_copy(n):
        i, p = n // 3, n % 3
        return pltpu.make_async_copy(gb.at[i % 2, p, half_of(c), :], own_ref.at[i, p], own_sem.at[i % 2, p])

    class Way:
        def __init__(self, d):
            self.d = d
            self.place = z if d == 0 else last - z
            self.step = 2 if d == 0 else -2
            self.small = pl.ds(d * quarter, quarter)
            self.block = 2 * d + c

        def loads(self, n):
            d, i, p = self.d, n // 3, n % 3
            return (
                pltpu.make_async_copy(own_ref.at[i, p, self.small, :], st.at[d, 0], ld_sem.at[d, 0]),
                pltpu.make_async_copy(pair_ref.at[i, p, self.small, :], st.at[d, 1], ld_sem.at[d, 1]),
                pltpu.make_async_copy(chain_ref.at[d, i, p], st.at[d, 2], ld_sem.at[d, 2]),
            )

        def hop(self, n):
            d, i, p = self.d, n // 3, n % 3
            return pltpu.make_async_remote_copy(
                src_ref=out.at[d, n % SLOTS], dst_ref=chain_ref.at[d, i, p], send_sem=chain_send.at[d, n % SLOTS], recv_sem=chain_recv.at[d, i, p],
                device_id={"dp": (dp + self.step) % (2 * CHIPS)}, device_id_type=MESH,
            )

        def keep(self, n):
            return pltpu.make_async_copy(out.at[self.d, n % SLOTS], g_ref.at[n // 3, n % 3, self.block], keep_sem.at[n % SLOTS])

        def spread(self, n):
            d, i, p = self.d, n // 3, n % 3
            return pltpu.make_async_remote_copy(
                src_ref=g_ref.at[i, p, self.block], dst_ref=g_ref.at[i, p, self.block], send_sem=pass_send.at[d, i, p], recv_sem=pass_recv.at[d, i, p],
                device_id={"dp": (dp - self.step + 2 * CHIPS) % (2 * CHIPS)}, device_id_type=MESH,
            )

        def share(self, n):
            d, i, p = self.d, n // 3, n % 3
            return pltpu.make_async_remote_copy(
                src_ref=g_ref.at[i, p, self.block], dst_ref=g_ref.at[i, p, self.block], send_sem=mate_send.at[d, i, p], recv_sem=mate_recv.at[d, i, p],
                device_id={"dp": mate}, device_id_type=MESH,
            )

        def reaches(self, n, place):
            return last - place <= WHOLE + last - 1 - n // 3

        def holds(self, n):
            return (self.place == last) | self.reaches(n, self.place)

        def passes(self, n):
            return (self.place > 0) & self.reaches(n, self.place - 1)

    ways = (Way(0), Way(1))

    def inside(n):
        return (n >= 0) & (n < UNITS)

    def unit(k):
        return jnp.where(k < 3 * PARTS, k, jnp.where(k < 3 * PARTS + PARTS, -1, k - PARTS))

    def start_tick(k):
        newest = unit(k - 2)

        @pl.when(inside(newest))
        def _():
            own_copy(newest).wait()
            pair_copy(newest).wait_recv()

        for way in ways:
            n = unit(k - 2 - LAG * way.place)

            @pl.when(inside(n))
            def _(way=way, n=n):
                own, pair, chain = way.loads(n)
                own.start()
                pair.start()

                @pl.when(way.place > 0)
                def _():
                    way.hop(n).wait_recv()
                    chain.start()

    def finish_tick(k):
        for way in ways:
            d = way.d
            n = unit(k - 2 - LAG * way.place)

            @pl.when(inside(n))
            def _(way=way, d=d, n=n):
                own, pair, chain = way.loads(n)
                own.wait()
                pair.wait()

                @pl.when((way.place < last) & (n >= SLOTS))
                def _():
                    way.hop(n - SLOTS).wait_send()

                def add(so_far):
                    wide = st[d, 0].astype(F32) + st[d, 1].astype(F32)
                    if so_far:
                        wide += st[d, 2].astype(F32)
                    rounded = wide.astype(BF16)
                    out[d, n % SLOTS] = rounded
                    return rounded.astype(F32)

                @pl.when(way.place == 0)
                def _():
                    add(False)
                    way.hop(n).start()

                @pl.when((way.place > 0) & (way.place < last))
                def _():
                    chain.wait()
                    add(True)
                    way.hop(n).start()

                @pl.when(way.place == last)
                def _():
                    chain.wait()
                    total = add(True)
                    way.keep(n).start()
                    ssq[...] += jnp.sum((total * total).reshape(quarter // 8, 8, FS), 0)

        for way in ways:
            n = unit(k - 3 - LAG * (2 * last - way.place))

            @pl.when(inside(n))
            def _(way=way, n=n):
                @pl.when(way.place == last)
                def _():
                    way.keep(n).wait()

                @pl.when((way.place < last) & way.holds(n))
                def _():
                    way.spread(n).wait_recv()

                @pl.when(way.passes(n))
                def _():
                    way.spread(n).start()

                @pl.when(way.holds(n))
                def _():
                    way.share(n).start()

    def dgu_copy(t):
        return pltpu.make_async_copy(dgu.at[t % 2], dgu_ref.at[t], dgu_sem.at[t % 2])

    def backward(t, tick, w, early):
        slot, half_slot = w % 2, t % 2
        fetched(w)

        @pl.when(w < 4 * PARTS - 1)
        def _():
            fetch(w + 1)

        if early:

            @pl.when((t >= 2) & (t < PARTS))
            def _():
                dgu_copy(t - 2).wait()

        def hidden_half(k):
            start_tick(tick + k)

            def tile(r):
                rows = rows_of(k * (T // RT // 2) + r, RT)
                gu = dot(a[rows, :], wgu[slot])
                dh = dot_nt(up[rows, :], wd[slot]).astype(BF16).astype(F32)
                gate, lift = gu[:, :FS], gu[:, FS:]
                s = jax.nn.sigmoid(gate)
                silu = gate * s
                hid[rows, :] = (silu * lift).astype(BF16)
                dgu[half_slot, rows, :FS] = (dh * lift * (s + silu * (1.0 - s))).astype(BF16)
                dgu[half_slot, rows, FS:] = (dh * silu).astype(BF16)

            repeat(T // RT // 2, tile)
            finish_tick(tick + k)

        repeat(2, hidden_half)

        if early:

            @pl.when(t < KEPT)
            def _():
                dgu_copy(t).start()

        @pl.when(t >= 2)
        def _():
            for p in range(3):
                pair_copy(3 * (t - 2) + p).wait_send()

        def down_half(k):
            rows = half_of(jnp.where(k == 0, 1 - c, c))
            gb[half_slot, 0, rows, :] = dot(upt[rows, :], hid[...]).astype(BF16)

            @pl.when(k == 0)
            def _():
                pair_copy(3 * t).start()

            @pl.when(k == 1)
            def _():
                own_copy(3 * t).start()

        repeat(2, down_half)

        def both_half(k):
            @pl.when(k == 1)
            def _():
                start_tick(tick + 2)

            rows = half_of(jnp.where(k == 0, 1 - c, c))
            both = dot(at[rows, :], dgu[half_slot]).astype(BF16)
            gb[half_slot, 1, rows, :] = both[:, :FS]
            gb[half_slot, 2, rows, :] = both[:, FS:]

            @pl.when(k == 0)
            def _():
                pair_copy(3 * t + 1).start()
                pair_copy(3 * t + 2).start()

            @pl.when(k == 1)
            def _():
                own_copy(3 * t + 1).start()
                own_copy(3 * t + 2).start()
                finish_tick(tick + 2)

        repeat(2, both_half)

    def dgu_load(s):
        return pltpu.make_async_copy(dgu_ref.at[s + KEPT - PARTS], dgu.at[s % 2], dgu_sem.at[s % 2])

    def sum_for_a(s):
        w = 2 * PARTS + s
        fetched(w)
        fetch(w + 1)

        @pl.when(s >= PARTS - KEPT)
        def _():
            dgu_load(s).wait()

        @pl.when((s >= 1) & (s < PARTS - 1))
        def _():
            dgu_load(s + 1).start()

        @pl.when(s == PARTS - 1)
        def _():
            load_h.start()

        start_tick(3 * PARTS + s)

        def tile(rows):
            acc[rows, :] = jnp.where(s > 0, acc[rows, :], 0.0) + dot_nt(dgu[s % 2, rows, :], wgu[w % 2])

        over_rows(T, RT, tile)
        finish_tick(3 * PARTS + s)

    def slice_of(i):
        @pl.when(i == PARTS)
        def _():
            reload_x.start()
            repeat(PARTS, sum_for_a)
            cross_layers()

        later = i >= PARTS
        backward(i, jnp.where(later, 3 * i + PARTS, 3 * i), jnp.where(later, i + 2 * PARTS, i + PARTS), True)

    repeat(NS, slice_of)

    def drain(k):
        start_tick(UNITS + PARTS + k)
        finish_tick(UNITS + PARTS + k)

    ticks = max(UNITS + 2 + LAG * last + 1, 3 * (WHOLE + last - 1) + 2 + LAG * 2 * last + 1)
    repeat(ticks - UNITS, drain)

    folded[...] = sum(ssq[:, k * FOLD : (k + 1) * FOLD] for k in range(FS // FOLD))

    def squares(k, slot):
        return pltpu.make_async_remote_copy(
            src_ref=folded, dst_ref=ssq_ref.at[slot], send_sem=ssq_send.at[k], recv_sem=ssq_recv.at[slot],
            device_id={"dp": (dp + k) % (2 * CHIPS)}, device_id_type=MESH,
        )

    def holder(slot):
        return 2 * last * (slot // 2) + slot % 2

    for slot in range(4):

        @pl.when(dp == holder(slot))
        def _(slot=slot):
            pltpu.make_async_copy(folded, ssq_ref.at[slot], io_sem.at[0]).start()
            for k in range(1, 2 * CHIPS):
                squares(k, slot).start()

    for p in range(3):
        pair_copy(3 * (NS - 2) + p).wait_send()
        pair_copy(3 * (NS - 1) + p).wait_send()

    for way in ways:

        @pl.when(way.place < last)
        def _(way=way):
            repeat(SLOTS, lambda k: way.hop(UNITS - SLOTS + k).wait_send())

        def close(n, way=way):
            @pl.when(way.passes(n))
            def _():
                way.spread(n).wait_send()

            @pl.when(way.holds(n))
            def _():
                way.share(n).wait()

        repeat(UNITS, close)

    first = WHOLE + jnp.where(c == 0, z, last - z) - 1
    loads, stores = [], []
    for p in range(3):
        for core in range(2):
            staged = wgu.at[p % 2, pl.ds(p // 2 * half + core * quarter, quarter), pl.ds(0, FS)]
            loads.append(pltpu.make_async_copy(g_ref.at[first, p, 2 * c + core], staged, w_sem.at[core, p]))
            stores.append(pltpu.make_async_copy(staged, sent_ref.at[0, p, core], w_sem.at[core, p]))
    for load in loads:
        load.start()
    for load, store in zip(loads, stores, strict=True):
        load.wait()
        store.start()
    for store in stores:
        store.wait()

    for slot in range(4):

        @pl.when(dp == holder(slot))
        def _(slot=slot):
            pltpu.make_async_copy(folded, ssq_ref.at[slot], io_sem.at[0]).wait()
            for k in range(1, 2 * CHIPS):
                squares(k, slot).wait_send()

        @pl.when(dp != holder(slot))
        def _(slot=slot):
            squares(0, slot).wait_recv()


def gradients(x, dy, w_gate, w_up, w_down):
    _, T, D = x.shape
    F = w_gate.shape[2]
    FS = F // PARTS
    RF, RT, RD = min(1024, T), min(512, T // 2), min(256, T)
    anywhere = pl.BlockSpec(memory_space=pl.ANY)
    dma = pltpu.SemaphoreType.DMA
    return pl.pallas_call(
        functools.partial(gradients_kernel, (T, D, FS, RF, RT, RD)),
        out_shape=(
            jax.ShapeDtypeStruct((NS, 3, 4, D // 4, FS), BF16),
            jax.ShapeDtypeStruct((NS, 3, D // 2, FS), BF16),
            jax.ShapeDtypeStruct((NS, 3, D // 2, FS), BF16),
            jax.ShapeDtypeStruct((2, NS, 3, D // 4, FS), BF16),
            jax.ShapeDtypeStruct((4, 8, FOLD), F32),
            jax.ShapeDtypeStruct((1, 3, 2, D // 4, FS), BF16),
            jax.ShapeDtypeStruct((T, D), BF16),
            jax.ShapeDtypeStruct((KEPT, T, 2 * FS), BF16),
        ),
        in_specs=[anywhere] * 5,
        out_specs=(anywhere,) * 8,
        scratch_shapes=[
            pltpu.VMEM((T, D), BF16),
            pltpu.VMEM((D, T), BF16),
            pltpu.VMEM((T, D), BF16),
            pltpu.VMEM((D, T), BF16),
            pltpu.VMEM((T, D), F32),
            pltpu.VMEM((2, D, 2 * FS), BF16),
            pltpu.VMEM((2, FS, D), BF16),
            pltpu.VMEM((T, FS), BF16),
            pltpu.VMEM((2, T, 2 * FS), BF16),
            pltpu.VMEM((2, 3, D, FS), BF16),
            pltpu.VMEM((2, 3, D // 4, FS), BF16),
            pltpu.VMEM((2, SLOTS, D // 4, FS), BF16),
            pltpu.VMEM((8, FS), F32),
            pltpu.VMEM((8, FOLD), F32),
            dma((2, 3)),
            dma((3,)),
            dma((2,)),
            dma((2, 3)),
            dma((2, 3)),
            dma((NS, 3)),
            dma((2, 3)),
            dma((2, SLOTS)),
            dma((2, NS, 3)),
            dma((SLOTS,)),
            dma((2, WHOLE + CHIPS, 3)),
            dma((2, WHOLE + CHIPS, 3)),
            dma((2, NS, 3)),
            dma((2, NS, 3)),
            dma((2 * CHIPS,)),
            dma((4,)),
        ],
        compiler_params=pltpu.CompilerParams(collective_id=0, has_side_effects=True, vmem_limit_bytes=66_000_000),
        name="gradients",
    )(x, dy, w_gate, w_up, w_down)


SUBS, DEEP = 4, 6


def adamw_kernel(count, work, n_in, aliased, *refs):
    refs = list(refs)

    def take(n):
        out, refs[:n] = refs[:n], []
        return out

    ssq_ref, g_ref = take(2)
    back = take(n_in)
    arrays = take(9)
    take(9 if aliased else 0)
    results = take(9)
    bufs, outs = take(9), take(9)
    gv, squares, g_sem, in_sem, out_sem, squares_sem = take(6)
    quarter, FS = gv.shape[2:]
    few, part = quarter // SUBS, FS // SUBS
    dp = lax.axis_index("dp")
    z, c = dp // 2, dp % 2
    total = SUBS * len(work)
    numbers = [4 * i + b for i, b, _ in work]
    cut = next((k for k in range(1, len(work)) if numbers[k] != numbers[k - 1] + 1), len(work))

    def here(k, source):
        return pltpu.make_async_copy(source, gv.at[k], g_sem.at[k])

    def fetch(k):
        i, b, came = work[k]
        place = z if b < 2 else CHIPS - 1 - z
        for p in range(CHIPS):
            if came[p] is None:

                @pl.when(place == p)
                def _():
                    here(k, g_ref.at[i, :, b]).start()

            else:
                for core in range(2):

                    @pl.when((place == p) & (c == core))
                    def _(at=came[p][0 if core == b // 2 else 1]):
                        here(k, back[at].at[0, :, b % 2]).start()

    def blocks(n):
        k, sub = n // SUBS, n % SUBS
        at = numbers[0] + k if cut == len(work) else jnp.where(k < cut, numbers[0] + k, numbers[cut] - cut + k)
        i, b = at // 4, at % 4
        layer, hidden, q = 1 - i // PARTS, i % PARTS, b % 2 * 2 + b // 2
        across = (layer, pl.ds(pl.multiple_of(q * quarter + sub * few, few), few), pl.ds(pl.multiple_of(hidden * FS, FS), FS))
        down = (layer, pl.ds(pl.multiple_of(hidden * FS + sub * part, part), part), pl.ds(pl.multiple_of(q * quarter, quarter), quarter))
        return across, across, down

    def copies(n, inward):
        slot, where = n % DEEP, blocks(n)
        if inward:
            return [pltpu.make_async_copy(arrays[k].at[where[k % 3]], bufs[k].at[slot], in_sem.at[slot]) for k in range(9)]
        return [pltpu.make_async_copy(outs[k].at[slot], results[k].at[where[k % 3]], out_sem.at[slot]) for k in range(9)]

    def start(n, inward):
        for copy in copies(n, inward):
            copy.start()

    def wait(n, inward):
        for copy in copies(n, inward):
            copy.wait()

    load_squares = pltpu.make_async_copy(ssq_ref, squares, squares_sem)
    load_squares.start()
    fetch(0)
    for n in range(min(DEEP - 1, total)):
        start(n, True)
    for k in range(1, len(work)):
        fetch(k)
    load_squares.wait()
    factor = jnp.minimum(1.0, 0.5 * lax.rsqrt(jnp.sum(squares[...]) / count + 1e-30))

    def piece(n, _):
        k, sub, slot = n // SUBS, n % SUBS, n % DEEP

        @pl.when(sub == 0)
        def _():
            here(k, g_ref.at[0, :, 0]).wait()

        @pl.when(n + DEEP - 1 < total)
        def _():
            start(n + DEEP - 1, True)

        wait(n, True)

        @pl.when(n >= DEEP)
        def _():
            wait(n - DEEP, False)

        def update(number, g):
            g = g * factor
            m = 0.9 * bufs[3 + number][slot] + 0.1 * g
            v = 0.95 * bufs[6 + number][slot] + 0.05 * g * g
            w = bufs[number][slot].astype(F32)
            outs[number][slot] = (w - 0.02 * (m * lax.rsqrt(v + 1e-8) + 0.1 * w)).astype(BF16)
            outs[3 + number][slot] = m
            outs[6 + number][slot] = v

        rows = pl.ds(pl.multiple_of(sub * few, few), few)
        update(0, gv[k, 1, rows, :].astype(F32))
        update(1, gv[k, 2, rows, :].astype(F32))
        update(2, gv[k, 0, :, pl.ds(pl.multiple_of(sub * part, part), part)].astype(F32).T)
        start(n, False)
        return 0

    lax.fori_loop(0, total, piece, 0)
    lax.fori_loop(max(total - DEEP, 0), total, lambda n, _: (wait(n, False), 0)[1], 0)


def adamw(ssq, g, arrays, results, listed, back):
    _, _, _, quarter, FS = g.shape
    anywhere = pl.BlockSpec(memory_space=pl.ANY)
    size = 3 * len(listed) * quarter * FS
    ins = [ssq, g, *back, *arrays, *(results or ())]
    shapes = [(DEEP, quarter // SUBS, FS)] * 2 + [(DEEP, FS // SUBS, quarter)]
    bufs = [pltpu.VMEM(shapes[k % 3], a.dtype) for k, a in enumerate(arrays)]
    return pl.pallas_call(
        functools.partial(adamw_kernel, float(g.size), listed, len(back), bool(results)),
        in_specs=[anywhere] * len(ins),
        out_specs=[anywhere] * 9,
        out_shape=[jax.ShapeDtypeStruct(a.shape, a.dtype) for a in arrays],
        input_output_aliases={len(ins) - 9 + k: k for k in range(9)} if results else {},
        scratch_shapes=[
            *bufs,
            *bufs,
            pltpu.VMEM((len(listed), 3, quarter, FS), BF16),
            pltpu.VMEM(ssq.shape, F32),
            pltpu.SemaphoreType.DMA((len(listed),)),
            pltpu.SemaphoreType.DMA((DEEP,)),
            pltpu.SemaphoreType.DMA((DEEP,)),
            pltpu.SemaphoreType.DMA,
        ],
        compiler_params=pltpu.CompilerParams(vmem_limit_bytes=66_000_000),
        cost_estimate=pl.CostEstimate(flops=16 * size, bytes_accessed=22 * size, transcendentals=size),
        name="adamw",
    )(*ins)


def load_kernel(i, g_ref, _, sent_ref, buf, sem):
    dp = lax.axis_index("dp")
    z, c = dp // 2, dp % 2

    @pl.when(z == (CHIPS - 1) * (1 - c))
    def _():
        pieces = buf.shape[0]
        loads = [pltpu.make_async_copy(g_ref.at[i, p, pl.ds(2 * c, 2)], buf.at[p], sem.at[0, p]) for p in range(pieces)]
        stores = [pltpu.make_async_copy(buf.at[p], sent_ref.at[0, p], sem.at[1, p]) for p in range(pieces)]
        for load in loads:
            load.start()
        for load, store in zip(loads, stores, strict=True):
            load.wait()
            store.start()
        for store in stores:
            store.wait()


def load(g, i, came):
    anywhere = pl.BlockSpec(memory_space=pl.ANY)
    return pl.pallas_call(
        functools.partial(load_kernel, i),
        in_specs=[anywhere, anywhere],
        out_specs=anywhere,
        out_shape=jax.ShapeDtypeStruct(came.shape, came.dtype),
        input_output_aliases={1: 0},
        scratch_shapes=[pltpu.VMEM(came.shape[1:], BF16), pltpu.SemaphoreType.DMA((2, 3))],
        compiler_params=pltpu.CompilerParams(vmem_limit_bytes=66_000_000),
        cost_estimate=pl.CostEstimate(flops=came.size, bytes_accessed=4 * came.size, transcendentals=0),
        name="load",
    )(g, came)


def finish(g, ssq, sent, arrays):
    last = CHIPS - 1
    stages = NS - WHOLE
    ready = [(i, b, (None,) * CHIPS) for i in range(WHOLE) for b in range(4)]
    first = min(6, 2 * WHOLE)
    spare = 4 * WHOLE - 2 * first
    more = [spare // (stages - 2) + (s < spare % (stages - 2)) for s in range(stages - 2)] + [0] * 2
    back, index, results = [], {}, None

    def units(u):
        came = tuple(index[u - p] if p < last and u >= p else None for p in range(CHIPS))
        return [(WHOLE + u, b, came) for b in range(4)]

    def update(results, listed):
        used = sorted({at for _, _, came in listed for pair in came if pair for at in pair})
        where = {at: k for k, at in enumerate(used)}
        listed = [(i, b, tuple(pair and tuple(where[at] for at in pair) for pair in came)) for i, b, came in listed]
        return adamw(ssq, g, arrays, results, listed, [back[at] for at in used])

    def device(place, core):
        return 2 * (place if core == 0 else last - place) + core

    pending = None
    for s in range(stages + 2):
        if s < stages:
            moves = [(device(p, core), device(p - 1, core)) for p in range(1, CHIPS) if s + p - 1 < stages for core in range(2)]
            newest = lax.ppermute(sent, "dp", moves)
        if pending is not None:
            back.append(lax.ppermute(*pending))
            pending = None
        many = first if s < 2 else more[s - 2]
        listed, ready = ready[:many], ready[many:]
        if s >= 2:
            listed = listed + units(s - 2)
        results = update(results, listed)
        if s < stages:
            sent = load(g, WHOLE + s + last, newest) if s + last < stages else newest
            index[s] = (len(back), len(back) + 1)
            back.append(sent)
            pending = (sent, "dp", [(to, to + 1 - 2 * (to % 2)) for _, to in moves])
    return results


def solution(mesh):
    def step(x, dy, *arrays):
        g, *_, ssq, sent, _, _ = gradients(x, dy, *arrays[:3])
        return tuple(finish(g, ssq, sent, arrays))

    return jax.shard_map(
        step,
        mesh=mesh,
        in_specs=(P(("rep", "dp"), None, None),) * 2 + (P(None, None, None),) * 9,
        out_specs=(P("rep", None, None),) * 9,
        check_vma=False,
    )
```

```python
import functools

import jax
import jax.numpy as jnp
from jax import lax
from jax.experimental import pallas as pl
from jax.experimental.pallas import tpu as pltpu
from jax.sharding import PartitionSpec as P


MESH = pl.DeviceIdType.MESH
CHIPS = 4
PARTS = 8
NS = 2 * PARTS
KEPT = PARTS - 2
WHOLE = 5
LATE = WHOLE + 1
LAG = 3
SLOTS = 4
FOLD = 128
F32, BF16 = jnp.float32, jnp.bfloat16


def dot(a, b):
    return jnp.dot(a, b, preferred_element_type=F32)


def dot_nt(a, b):
    return lax.dot_general(a, b, (((1,), (1,)), ((), ())), preferred_element_type=F32)


def inverse_size(wide):
    return lax.rsqrt(jnp.mean(wide * wide, -1, keepdims=True) + 1e-6)


def gradients_kernel(
    sizes,
    x_ref, dy_ref, wg_ref, wu_ref, wd_ref,
    g_ref, own_ref, pair_ref, chain_ref, ssq_ref, sent_ref, h_ref, dgu_ref,
    a, at, up, upt, acc, wgu, wd, hid, dgu, gb, st, out, ssq, folded,
    w_sem, io_sem, dgu_sem, pair_send, own_sem, pair_recv, ld_sem, chain_send, chain_recv, keep_sem, pass_send, pass_recv, mate_send, mate_recv, ssq_send, ssq_recv,
):
    T, D, FS, RF, RT, RD = sizes
    UNITS = 3 * NS
    half, quarter = D // 2, D // 4
    dp = lax.axis_index("dp")
    z, c = dp // 2, dp % 2
    mate = dp + 1 - 2 * c
    last = CHIPS - 1

    barrier = pltpu.get_barrier_semaphore()
    for k in range(1, 2 * CHIPS):
        pl.semaphore_signal(barrier, inc=1, device_id={"dp": (dp + k) % (2 * CHIPS)}, device_id_type=MESH)

    def weight_copies(w):
        phase = w // PARTS
        layer = jnp.where((phase == 1) | (phase == 2), 1, 0)
        part = jnp.where(phase == 2, w + KEPT, w) % PARTS
        columns = pl.ds(pl.multiple_of(part * FS, FS), FS)
        slot = w % 2
        both = (
            pltpu.make_async_copy(wg_ref.at[layer, :, columns], wgu.at[slot, :, pl.ds(0, FS)], w_sem.at[slot, 0]),
            pltpu.make_async_copy(wu_ref.at[layer, :, columns], wgu.at[slot, :, pl.ds(FS, FS)], w_sem.at[slot, 1]),
        )
        return both, pltpu.make_async_copy(wd_ref.at[layer, columns, :], wd.at[slot], w_sem.at[slot, 2]), phase != 2

    def fetch(w):
        both, down, needed = weight_copies(w)
        for copy in both:
            copy.start()

        @pl.when(needed)
        def _():
            down.start()

    def fetched(w):
        both, down, needed = weight_copies(w)
        for copy in both:
            copy.wait()

        @pl.when(needed)
        def _():
            down.wait()

    def rows_of(r, size):
        return pl.ds(pl.multiple_of(r * size, size), size)

    def repeat(n, body):
        lax.fori_loop(0, n, lambda r, _: (body(r), 0)[1], 0)

    def over_rows(total, size, body):
        repeat(total // size, lambda r: body(rows_of(r, size)))

    load_x = pltpu.make_async_copy(x_ref.at[0], a, io_sem.at[0])
    load_x.start()
    fetch(0)
    load_again = pltpu.make_async_copy(x_ref.at[0], dgu.at[0], io_sem.at[1])
    load_again.start()
    load_dy = pltpu.make_async_copy(dy_ref.at[0], up, io_sem.at[2])
    load_dy.start()
    ssq[...] = jnp.zeros_like(ssq)
    load_x.wait()

    def norm_in_place(rows):
        wide = a[rows, :].astype(F32)
        a[rows, :] = (wide * inverse_size(wide)).astype(BF16)

    over_rows(T, RD, norm_in_place)

    def forward(j):
        slot = j % 2
        fetched(j)
        fetch(j + 1)

        def tile(rows):
            gu = dot(a[rows, :], wgu[slot])
            gate, lift = gu[:, :FS], gu[:, FS:]
            hidden = (gate * jax.nn.sigmoid(gate) * lift).astype(BF16)
            acc[rows, :] = jnp.where(j > 0, acc[rows, :], 0.0) + dot(hidden, wd[slot])

        over_rows(T, RF, tile)

    repeat(PARTS, forward)

    load_again.wait()
    load_dy.wait()

    def close_forward(rows):
        h = dgu[0, rows, :].astype(F32) + acc[rows, :].astype(BF16).astype(F32)
        h = h.astype(BF16)
        dgu[0, rows, :] = h
        wide = h.astype(F32)
        normed = (wide * inverse_size(wide)).astype(BF16)
        a[rows, :] = normed
        at[:, rows] = normed.T
        upt[:, rows] = up[rows, :].T

    over_rows(T, RD, close_forward)
    save_h = pltpu.make_async_copy(dgu.at[0], h_ref, io_sem.at[0])
    save_h.start()
    pl.semaphore_wait(barrier, 2 * CHIPS - 1)
    save_h.wait()

    reload_x = pltpu.make_async_copy(x_ref.at[0], a, io_sem.at[1])
    load_h = pltpu.make_async_copy(h_ref, dgu.at[0], io_sem.at[0])

    def cross_layers():
        reload_x.wait()
        load_h.wait()

        def tile(rows):
            wide = a[rows, :].astype(F32)
            normed = (wide * inverse_size(wide)).astype(BF16)
            a[rows, :] = normed
            at[:, rows] = normed.T
            wide = dgu[0, rows, :].astype(F32)
            scale = inverse_size(wide)
            da = acc[rows, :].astype(BF16).astype(F32)
            along = jnp.sum(da * wide, -1, keepdims=True) * (1.0 / D)
            dh = (scale * da - wide * (scale * scale * scale * along)).astype(BF16)
            new = (up[rows, :].astype(F32) + dh.astype(F32)).astype(BF16)
            up[rows, :] = new
            upt[:, rows] = new.T

        over_rows(T, RD, tile)

    def half_of(core):
        return pl.ds(pl.multiple_of(core * half, half), half)

    def pair_copy(n):
        i, p = n // 3, n % 3
        return pltpu.make_async_remote_copy(
            src_ref=gb.at[i % 2, p, half_of(1 - c), :], dst_ref=pair_ref.at[i, p], send_sem=pair_send.at[i % 2, p], recv_sem=pair_recv.at[i, p],
            device_id={"dp": mate}, device_id_type=MESH,
        )

    def own_copy(n):
        i, p = n // 3, n % 3
        return pltpu.make_async_copy(gb.at[i % 2, p, half_of(c), :], own_ref.at[i, p], own_sem.at[i % 2, p])

    class Way:
        def __init__(self, d):
            self.d = d
            self.place = z if d == 0 else last - z
            self.step = 2 if d == 0 else -2
            self.small = pl.ds(d * quarter, quarter)
            self.block = 2 * d + c

        def loads(self, n):
            d, i, p = self.d, n // 3, n % 3
            return (
                pltpu.make_async_copy(own_ref.at[i, p, self.small, :], st.at[d, 0], ld_sem.at[d, 0]),
                pltpu.make_async_copy(pair_ref.at[i, p, self.small, :], st.at[d, 1], ld_sem.at[d, 1]),
                pltpu.make_async_copy(chain_ref.at[d, i, p], st.at[d, 2], ld_sem.at[d, 2]),
            )

        def hop(self, n):
            d, i, p = self.d, n // 3, n % 3
            return pltpu.make_async_remote_copy(
                src_ref=out.at[d, n % SLOTS], dst_ref=chain_ref.at[d, i, p], send_sem=chain_send.at[d, n % SLOTS], recv_sem=chain_recv.at[d, i, p],
                device_id={"dp": (dp + self.step) % (2 * CHIPS)}, device_id_type=MESH,
            )

        def keep(self, n):
            return pltpu.make_async_copy(out.at[self.d, n % SLOTS], g_ref.at[n // 3, n % 3, self.block], keep_sem.at[n % SLOTS])

        def spread(self, n):
            d, i, p = self.d, n // 3, n % 3
            return pltpu.make_async_remote_copy(
                src_ref=g_ref.at[i, p, self.block], dst_ref=g_ref.at[i, p, self.block], send_sem=pass_send.at[d, i, p], recv_sem=pass_recv.at[d, i, p],
                device_id={"dp": (dp - self.step + 2 * CHIPS) % (2 * CHIPS)}, device_id_type=MESH,
            )

        def share(self, n):
            d, i, p = self.d, n // 3, n % 3
            return pltpu.make_async_remote_copy(
                src_ref=g_ref.at[i, p, self.block], dst_ref=g_ref.at[i, p, self.block], send_sem=mate_send.at[d, i, p], recv_sem=mate_recv.at[d, i, p],
                device_id={"dp": mate}, device_id_type=MESH,
            )

        def reaches(self, n, place):
            return last - place <= WHOLE + last - 1 - n // 3

        def holds(self, n):
            return (self.place == last) | self.reaches(n, self.place)

        def passes(self, n):
            return (self.place > 0) & self.reaches(n, self.place - 1)

    ways = (Way(0), Way(1))

    def inside(n):
        return (n >= 0) & (n < UNITS)

    def unit(k):
        return jnp.where(k < 3 * PARTS, k, jnp.where(k < 3 * PARTS + PARTS, -1, k - PARTS))

    def start_tick(k):
        newest = unit(k - 2)

        @pl.when(inside(newest))
        def _():
            own_copy(newest).wait()
            pair_copy(newest).wait_recv()

        for way in ways:
            n = unit(k - 2 - LAG * way.place)

            @pl.when(inside(n))
            def _(way=way, n=n):
                own, pair, chain = way.loads(n)
                own.start()
                pair.start()

                @pl.when(way.place > 0)
                def _():
                    way.hop(n).wait_recv()
                    chain.start()

    def finish_tick(k):
        for way in ways:
            d = way.d
            n = unit(k - 2 - LAG * way.place)

            @pl.when(inside(n))
            def _(way=way, d=d, n=n):
                own, pair, chain = way.loads(n)
                own.wait()
                pair.wait()

                @pl.when((way.place < last) & (n >= SLOTS))
                def _():
                    way.hop(n - SLOTS).wait_send()

                def add(so_far):
                    wide = st[d, 0].astype(F32) + st[d, 1].astype(F32)
                    if so_far:
                        wide += st[d, 2].astype(F32)
                    rounded = wide.astype(BF16)
                    out[d, n % SLOTS] = rounded
                    return rounded.astype(F32)

                @pl.when(way.place == 0)
                def _():
                    add(False)
                    way.hop(n).start()

                @pl.when((way.place > 0) & (way.place < last))
                def _():
                    chain.wait()
                    add(True)
                    way.hop(n).start()

                @pl.when(way.place == last)
                def _():
                    chain.wait()
                    total = add(True)
                    way.keep(n).start()
                    ssq[...] += jnp.sum((total * total).reshape(quarter // 8, 8, FS), 0)

        for way in ways:
            n = unit(k - 3 - LAG * (2 * last - way.place))

            @pl.when(inside(n))
            def _(way=way, n=n):
                @pl.when(way.place == last)
                def _():
                    way.keep(n).wait()

                on_time = n // 3 != LATE

                @pl.when((way.place < last) & way.holds(n) & on_time)
                def _():
                    way.spread(n).wait_recv()

                @pl.when(way.passes(n) & on_time)
                def _():
                    way.spread(n).start()

                @pl.when(way.holds(n) & ((way.place == last) | on_time))
                def _():
                    way.share(n).start()

            m = k - (UNITS + PARTS + 2) - LAG * (last - way.place)

            @pl.when((m >= 0) & (m < 3) & (way.place >= last - 1))
            def _(way=way, m=m):
                n = 3 * LATE + m

                @pl.when(way.place == last)
                def _():
                    way.spread(n).start()

                @pl.when(way.place < last)
                def _():
                    way.spread(n).wait_recv()
                    way.share(n).start()

    def dgu_copy(t):
        return pltpu.make_async_copy(dgu.at[t % 2], dgu_ref.at[t], dgu_sem.at[t % 2])

    def backward(t, tick, w, early):
        slot, half_slot = w % 2, t % 2
        fetched(w)

        @pl.when(w < 4 * PARTS - 1)
        def _():
            fetch(w + 1)

        if early:

            @pl.when((t >= 2) & (t < PARTS))
            def _():
                dgu_copy(t - 2).wait()

        def hidden_half(k):
            start_tick(tick + k)

            def tile(r):
                rows = rows_of(k * (T // RT // 2) + r, RT)
                gu = dot(a[rows, :], wgu[slot])
                dh = dot_nt(up[rows, :], wd[slot]).astype(BF16).astype(F32)
                gate, lift = gu[:, :FS], gu[:, FS:]
                s = jax.nn.sigmoid(gate)
                silu = gate * s
                hid[rows, :] = (silu * lift).astype(BF16)
                dgu[half_slot, rows, :FS] = (dh * lift * (s + silu * (1.0 - s))).astype(BF16)
                dgu[half_slot, rows, FS:] = (dh * silu).astype(BF16)

            repeat(T // RT // 2, tile)
            finish_tick(tick + k)

        repeat(2, hidden_half)

        if early:

            @pl.when(t < KEPT)
            def _():
                dgu_copy(t).start()

        @pl.when(t >= 2)
        def _():
            for p in range(3):
                pair_copy(3 * (t - 2) + p).wait_send()

        def down_half(k):
            rows = half_of(jnp.where(k == 0, 1 - c, c))
            gb[half_slot, 0, rows, :] = dot(upt[rows, :], hid[...]).astype(BF16)

            @pl.when(k == 0)
            def _():
                pair_copy(3 * t).start()

            @pl.when(k == 1)
            def _():
                own_copy(3 * t).start()

        repeat(2, down_half)

        def both_half(k):
            @pl.when(k == 1)
            def _():
                start_tick(tick + 2)

            rows = half_of(jnp.where(k == 0, 1 - c, c))
            both = dot(at[rows, :], dgu[half_slot]).astype(BF16)
            gb[half_slot, 1, rows, :] = both[:, :FS]
            gb[half_slot, 2, rows, :] = both[:, FS:]

            @pl.when(k == 0)
            def _():
                pair_copy(3 * t + 1).start()
                pair_copy(3 * t + 2).start()

            @pl.when(k == 1)
            def _():
                own_copy(3 * t + 1).start()
                own_copy(3 * t + 2).start()
                finish_tick(tick + 2)

        repeat(2, both_half)

    def dgu_load(s):
        return pltpu.make_async_copy(dgu_ref.at[s + KEPT - PARTS], dgu.at[s % 2], dgu_sem.at[s % 2])

    def sum_for_a(s):
        w = 2 * PARTS + s
        fetched(w)
        fetch(w + 1)

        @pl.when(s >= PARTS - KEPT)
        def _():
            dgu_load(s).wait()

        @pl.when((s >= 1) & (s < PARTS - 1))
        def _():
            dgu_load(s + 1).start()

        @pl.when(s == PARTS - 1)
        def _():
            load_h.start()

        start_tick(3 * PARTS + s)

        def tile(rows):
            acc[rows, :] = jnp.where(s > 0, acc[rows, :], 0.0) + dot_nt(dgu[s % 2, rows, :], wgu[w % 2])

        over_rows(T, RT, tile)
        finish_tick(3 * PARTS + s)

    def slice_of(i):
        @pl.when(i == PARTS)
        def _():
            reload_x.start()
            repeat(PARTS, sum_for_a)
            cross_layers()

        later = i >= PARTS
        backward(i, jnp.where(later, 3 * i + PARTS, 3 * i), jnp.where(later, i + 2 * PARTS, i + PARTS), True)

    repeat(NS, slice_of)

    def drain(k):
        start_tick(UNITS + PARTS + k)
        finish_tick(UNITS + PARTS + k)

    ticks = max(UNITS + 2 + LAG * last + 1, 3 * (WHOLE + last - 1) + 2 + LAG * 2 * last + 1)
    repeat(ticks - UNITS, drain)

    folded[...] = sum(ssq[:, k * FOLD : (k + 1) * FOLD] for k in range(FS // FOLD))

    def squares(k, slot):
        return pltpu.make_async_remote_copy(
            src_ref=folded, dst_ref=ssq_ref.at[slot], send_sem=ssq_send.at[k], recv_sem=ssq_recv.at[slot],
            device_id={"dp": (dp + k) % (2 * CHIPS)}, device_id_type=MESH,
        )

    def holder(slot):
        return 2 * last * (slot // 2) + slot % 2

    for slot in range(4):

        @pl.when(dp == holder(slot))
        def _(slot=slot):
            pltpu.make_async_copy(folded, ssq_ref.at[slot], io_sem.at[0]).start()
            for k in range(1, 2 * CHIPS):
                squares(k, slot).start()

    for p in range(3):
        pair_copy(3 * (NS - 2) + p).wait_send()
        pair_copy(3 * (NS - 1) + p).wait_send()

    for way in ways:

        @pl.when(way.place < last)
        def _(way=way):
            repeat(SLOTS, lambda k: way.hop(UNITS - SLOTS + k).wait_send())

        def close(n, way=way):
            @pl.when(way.passes(n))
            def _():
                way.spread(n).wait_send()

            @pl.when(way.holds(n))
            def _():
                way.share(n).wait()

        repeat(UNITS, close)

    first = WHOLE + jnp.where(c == 0, z, last - z) - 1
    loads, stores = [], []
    for p in range(3):
        for core in range(2):
            staged = wgu.at[p % 2, pl.ds(p // 2 * half + core * quarter, quarter), pl.ds(0, FS)]
            loads.append(pltpu.make_async_copy(g_ref.at[first, p, 2 * c + core], staged, w_sem.at[core, p]))
            stores.append(pltpu.make_async_copy(staged, sent_ref.at[0, p, core], w_sem.at[core, p]))
    for load in loads:
        load.start()
    for load, store in zip(loads, stores, strict=True):
        load.wait()
        store.start()
    for store in stores:
        store.wait()

    for slot in range(4):

        @pl.when(dp == holder(slot))
        def _(slot=slot):
            pltpu.make_async_copy(folded, ssq_ref.at[slot], io_sem.at[0]).wait()
            for k in range(1, 2 * CHIPS):
                squares(k, slot).wait_send()

        @pl.when(dp != holder(slot))
        def _(slot=slot):
            squares(0, slot).wait_recv()


def gradients(x, dy, w_gate, w_up, w_down):
    _, T, D = x.shape
    F = w_gate.shape[2]
    FS = F // PARTS
    RF, RT, RD = min(1024, T), min(1024, T // 2), min(256, T)
    anywhere = pl.BlockSpec(memory_space=pl.ANY)
    dma = pltpu.SemaphoreType.DMA
    return pl.pallas_call(
        functools.partial(gradients_kernel, (T, D, FS, RF, RT, RD)),
        out_shape=(
            jax.ShapeDtypeStruct((NS, 3, 4, D // 4, FS), BF16),
            jax.ShapeDtypeStruct((NS, 3, D // 2, FS), BF16),
            jax.ShapeDtypeStruct((NS, 3, D // 2, FS), BF16),
            jax.ShapeDtypeStruct((2, NS, 3, D // 4, FS), BF16),
            jax.ShapeDtypeStruct((4, 8, FOLD), F32),
            jax.ShapeDtypeStruct((1, 3, 2, D // 4, FS), BF16),
            jax.ShapeDtypeStruct((T, D), BF16),
            jax.ShapeDtypeStruct((KEPT, T, 2 * FS), BF16),
        ),
        in_specs=[anywhere] * 5,
        out_specs=(anywhere,) * 8,
        scratch_shapes=[
            pltpu.VMEM((T, D), BF16),
            pltpu.VMEM((D, T), BF16),
            pltpu.VMEM((T, D), BF16),
            pltpu.VMEM((D, T), BF16),
            pltpu.VMEM((T, D), F32),
            pltpu.VMEM((2, D, 2 * FS), BF16),
            pltpu.VMEM((2, FS, D), BF16),
            pltpu.VMEM((T, FS), BF16),
            pltpu.VMEM((2, T, 2 * FS), BF16),
            pltpu.VMEM((2, 3, D, FS), BF16),
            pltpu.VMEM((2, 3, D // 4, FS), BF16),
            pltpu.VMEM((2, SLOTS, D // 4, FS), BF16),
            pltpu.VMEM((8, FS), F32),
            pltpu.VMEM((8, FOLD), F32),
            dma((2, 3)),
            dma((3,)),
            dma((2,)),
            dma((2, 3)),
            dma((2, 3)),
            dma((NS, 3)),
            dma((2, 3)),
            dma((2, SLOTS)),
            dma((2, NS, 3)),
            dma((SLOTS,)),
            dma((2, WHOLE + CHIPS, 3)),
            dma((2, WHOLE + CHIPS, 3)),
            dma((2, NS, 3)),
            dma((2, NS, 3)),
            dma((2 * CHIPS,)),
            dma((4,)),
        ],
        compiler_params=pltpu.CompilerParams(collective_id=0, has_side_effects=True, vmem_limit_bytes=66_000_000),
        name="gradients",
    )(x, dy, w_gate, w_up, w_down)


SUBS, DEEP = 4, 6


def adamw_kernel(count, work, n_in, aliased, *refs):
    refs = list(refs)

    def take(n):
        out, refs[:n] = refs[:n], []
        return out

    ssq_ref, g_ref = take(2)
    back = take(n_in)
    arrays = take(9)
    take(9 if aliased else 0)
    results = take(9)
    bufs, outs = take(9), take(9)
    gv, squares, g_sem, in_sem, out_sem, squares_sem = take(6)
    quarter, FS = gv.shape[2:]
    few, part = quarter // SUBS, FS // SUBS
    dp = lax.axis_index("dp")
    z, c = dp // 2, dp % 2
    total = SUBS * len(work)
    numbers = [4 * i + b for i, b, _ in work]
    cut = next((k for k in range(1, len(work)) if numbers[k] != numbers[k - 1] + 1), len(work))

    def here(k, source):
        return pltpu.make_async_copy(source, gv.at[k], g_sem.at[k])

    def fetch(k):
        i, b, came = work[k]
        place = z if b < 2 else CHIPS - 1 - z
        for p in range(CHIPS):
            if came[p] is None:

                @pl.when(place == p)
                def _():
                    here(k, g_ref.at[i, :, b]).start()

            else:
                for core in range(2):

                    @pl.when((place == p) & (c == core))
                    def _(at=came[p][0 if core == b // 2 else 1]):
                        here(k, back[at].at[0, :, b % 2]).start()

    def blocks(n):
        k, sub = n // SUBS, n % SUBS
        at = numbers[0] + k if cut == len(work) else jnp.where(k < cut, numbers[0] + k, numbers[cut] - cut + k)
        i, b = at // 4, at % 4
        layer, hidden, q = 1 - i // PARTS, i % PARTS, b % 2 * 2 + b // 2
        across = (layer, pl.ds(pl.multiple_of(q * quarter + sub * few, few), few), pl.ds(pl.multiple_of(hidden * FS, FS), FS))
        down = (layer, pl.ds(pl.multiple_of(hidden * FS + sub * part, part), part), pl.ds(pl.multiple_of(q * quarter, quarter), quarter))
        return across, across, down

    def copies(n, inward):
        slot, where = n % DEEP, blocks(n)
        if inward:
            return [pltpu.make_async_copy(arrays[k].at[where[k % 3]], bufs[k].at[slot], in_sem.at[slot]) for k in range(9)]
        return [pltpu.make_async_copy(outs[k].at[slot], results[k].at[where[k % 3]], out_sem.at[slot]) for k in range(9)]

    def start(n, inward):
        for copy in copies(n, inward):
            copy.start()

    def wait(n, inward):
        for copy in copies(n, inward):
            copy.wait()

    load_squares = pltpu.make_async_copy(ssq_ref, squares, squares_sem)
    load_squares.start()
    fetch(0)
    for n in range(min(DEEP - 1, total)):
        start(n, True)
    for k in range(1, len(work)):
        fetch(k)
    load_squares.wait()
    factor = jnp.minimum(1.0, 0.5 * lax.rsqrt(jnp.sum(squares[...]) / count + 1e-30))

    def piece(n, _):
        k, sub, slot = n // SUBS, n % SUBS, n % DEEP

        @pl.when(sub == 0)
        def _():
            here(k, g_ref.at[0, :, 0]).wait()

        @pl.when(n + DEEP - 1 < total)
        def _():
            start(n + DEEP - 1, True)

        wait(n, True)

        @pl.when(n >= DEEP)
        def _():
            wait(n - DEEP, False)

        def update(number, g):
            g = g * factor
            m = 0.9 * bufs[3 + number][slot] + 0.1 * g
            v = 0.95 * bufs[6 + number][slot] + 0.05 * g * g
            w = bufs[number][slot].astype(F32)
            outs[number][slot] = (w - 0.02 * (m * lax.rsqrt(v + 1e-8) + 0.1 * w)).astype(BF16)
            outs[3 + number][slot] = m
            outs[6 + number][slot] = v

        rows = pl.ds(pl.multiple_of(sub * few, few), few)
        update(0, gv[k, 1, rows, :].astype(F32))
        update(1, gv[k, 2, rows, :].astype(F32))
        update(2, gv[k, 0, :, pl.ds(pl.multiple_of(sub * part, part), part)].astype(F32).T)
        start(n, False)
        return 0

    lax.fori_loop(0, total, piece, 0)
    lax.fori_loop(max(total - DEEP, 0), total, lambda n, _: (wait(n, False), 0)[1], 0)


def adamw(ssq, g, arrays, results, listed, back):
    _, _, _, quarter, FS = g.shape
    anywhere = pl.BlockSpec(memory_space=pl.ANY)
    size = 3 * len(listed) * quarter * FS
    ins = [ssq, g, *back, *arrays, *(results or ())]
    shapes = [(DEEP, quarter // SUBS, FS)] * 2 + [(DEEP, FS // SUBS, quarter)]
    bufs = [pltpu.VMEM(shapes[k % 3], a.dtype) for k, a in enumerate(arrays)]
    return pl.pallas_call(
        functools.partial(adamw_kernel, float(g.size), listed, len(back), bool(results)),
        in_specs=[anywhere] * len(ins),
        out_specs=[anywhere] * 9,
        out_shape=[jax.ShapeDtypeStruct(a.shape, a.dtype) for a in arrays],
        input_output_aliases={len(ins) - 9 + k: k for k in range(9)} if results else {},
        scratch_shapes=[
            *bufs,
            *bufs,
            pltpu.VMEM((len(listed), 3, quarter, FS), BF16),
            pltpu.VMEM(ssq.shape, F32),
            pltpu.SemaphoreType.DMA((len(listed),)),
            pltpu.SemaphoreType.DMA((DEEP,)),
            pltpu.SemaphoreType.DMA((DEEP,)),
            pltpu.SemaphoreType.DMA,
        ],
        compiler_params=pltpu.CompilerParams(vmem_limit_bytes=66_000_000),
        cost_estimate=pl.CostEstimate(flops=16 * size, bytes_accessed=22 * size, transcendentals=size),
        name="adamw",
    )(*ins)


def load_kernel(i, g_ref, _, sent_ref, buf, sem):
    dp = lax.axis_index("dp")
    z, c = dp // 2, dp % 2

    @pl.when(z == (CHIPS - 1) * (1 - c))
    def _():
        pieces = buf.shape[0]
        loads = [pltpu.make_async_copy(g_ref.at[i, p, pl.ds(2 * c, 2)], buf.at[p], sem.at[0, p]) for p in range(pieces)]
        stores = [pltpu.make_async_copy(buf.at[p], sent_ref.at[0, p], sem.at[1, p]) for p in range(pieces)]
        for load in loads:
            load.start()
        for load, store in zip(loads, stores, strict=True):
            load.wait()
            store.start()
        for store in stores:
            store.wait()


def load(g, i, came):
    anywhere = pl.BlockSpec(memory_space=pl.ANY)
    return pl.pallas_call(
        functools.partial(load_kernel, i),
        in_specs=[anywhere, anywhere],
        out_specs=anywhere,
        out_shape=jax.ShapeDtypeStruct(came.shape, came.dtype),
        input_output_aliases={1: 0},
        scratch_shapes=[pltpu.VMEM(came.shape[1:], BF16), pltpu.SemaphoreType.DMA((2, 3))],
        compiler_params=pltpu.CompilerParams(vmem_limit_bytes=66_000_000),
        cost_estimate=pl.CostEstimate(flops=came.size, bytes_accessed=4 * came.size, transcendentals=0),
        name="load",
    )(g, came)


def finish(g, ssq, sent, arrays):
    last = CHIPS - 1
    stages = NS - WHOLE
    ready = [(i, b, (None,) * CHIPS) for i in range(WHOLE) for b in range(4)]
    first = min(6, 2 * WHOLE)
    spare = 4 * WHOLE - 2 * first
    more = [spare // (stages - 2) + (s < spare % (stages - 2)) for s in range(stages - 2)] + [0] * 2
    back, index, results = [], {}, None

    def units(u):
        came = tuple(index[u - p] if p < last and u >= p else None for p in range(CHIPS))
        return [(WHOLE + u, b, came) for b in range(4)]

    def update(results, listed):
        used = sorted({at for _, _, came in listed for pair in came if pair for at in pair})
        where = {at: k for k, at in enumerate(used)}
        listed = [(i, b, tuple(pair and tuple(where[at] for at in pair) for pair in came)) for i, b, came in listed]
        return adamw(ssq, g, arrays, results, listed, [back[at] for at in used])

    def device(place, core):
        return 2 * (place if core == 0 else last - place) + core

    pending = None
    for s in range(stages + 2):
        if s < stages:
            moves = [(device(p, core), device(p - 1, core)) for p in range(1, CHIPS) if s + p - 1 < stages for core in range(2)]
            newest = lax.ppermute(sent, "dp", moves)
        if pending is not None:
            back.append(lax.ppermute(*pending))
            pending = None
        many = first if s < 2 else more[s - 2]
        listed, ready = ready[:many], ready[many:]
        if s >= 2:
            listed = listed + units(s - 2)
        results = update(results, listed)
        if s < stages:
            sent = load(g, WHOLE + s + last, newest) if s + last < stages else newest
            index[s] = (len(back), len(back) + 1)
            back.append(sent)
            pending = (sent, "dp", [(to, to + 1 - 2 * (to % 2)) for _, to in moves])
    return results


def solution(mesh):
    def step(x, dy, *arrays):
        g, *_, ssq, sent, _, _ = gradients(x, dy, *arrays[:3])
        return tuple(finish(g, ssq, sent, arrays))

    return jax.shard_map(
        step,
        mesh=mesh,
        in_specs=(P(("rep", "dp"), None, None),) * 2 + (P(None, None, None),) * 9,
        out_specs=(P("rep", None, None),) * 9,
        check_vma=False,
    )
```

```python
import functools

import jax
import jax.numpy as jnp
from jax import lax
from jax.experimental import pallas as pl
from jax.experimental.pallas import tpu as pltpu
from jax.sharding import PartitionSpec as P


MESH = pl.DeviceIdType.MESH
CHIPS = 4
PARTS = 8
NS = 2 * PARTS
KEPT = PARTS - 2
WHOLE = 6
LAG = 3
SLOTS = 4
FOLD = 128
F32, BF16 = jnp.float32, jnp.bfloat16


def dot(a, b):
    return jnp.dot(a, b, preferred_element_type=F32)


def dot_nt(a, b):
    return lax.dot_general(a, b, (((1,), (1,)), ((), ())), preferred_element_type=F32)


def inverse_size(wide):
    return lax.rsqrt(jnp.mean(wide * wide, -1, keepdims=True) + 1e-6)


def gradients_kernel(
    sizes,
    x_ref, dy_ref, wg_ref, wu_ref, wd_ref,
    g_ref, own_ref, pair_ref, chain_ref, ssq_ref, sent_ref, h_ref, dgu_ref,
    a, at, up, upt, acc, wgu, wd, hid, dgu, gb, st, out, ssq, folded,
    w_sem, io_sem, dgu_sem, pair_send, own_sem, pair_recv, ld_sem, chain_send, chain_recv, keep_sem, pass_send, pass_recv, mate_send, mate_recv, ssq_send, ssq_recv,
):
    T, D, FS, RF, RT, RD = sizes
    UNITS = 3 * NS
    half, quarter = D // 2, D // 4
    dp = lax.axis_index("dp")
    z, c = dp // 2, dp % 2
    mate = dp + 1 - 2 * c
    last = CHIPS - 1

    barrier = pltpu.get_barrier_semaphore()
    for k in range(1, 2 * CHIPS):
        pl.semaphore_signal(barrier, inc=1, device_id={"dp": (dp + k) % (2 * CHIPS)}, device_id_type=MESH)

    def weight_copies(w):
        phase = w // PARTS
        layer = jnp.where((phase == 1) | (phase == 2), 1, 0)
        part = jnp.where(phase == 2, w + KEPT, w) % PARTS
        columns = pl.ds(pl.multiple_of(part * FS, FS), FS)
        slot = w % 2
        both = (
            pltpu.make_async_copy(wg_ref.at[layer, :, columns], wgu.at[slot, :, pl.ds(0, FS)], w_sem.at[slot, 0]),
            pltpu.make_async_copy(wu_ref.at[layer, :, columns], wgu.at[slot, :, pl.ds(FS, FS)], w_sem.at[slot, 1]),
        )
        return both, pltpu.make_async_copy(wd_ref.at[layer, columns, :], wd.at[slot], w_sem.at[slot, 2]), phase != 2

    def fetch(w):
        both, down, needed = weight_copies(w)
        for copy in both:
            copy.start()

        @pl.when(needed)
        def _():
            down.start()

    def fetched(w):
        both, down, needed = weight_copies(w)
        for copy in both:
            copy.wait()

        @pl.when(needed)
        def _():
            down.wait()

    def rows_of(r, size):
        return pl.ds(pl.multiple_of(r * size, size), size)

    def repeat(n, body):
        lax.fori_loop(0, n, lambda r, _: (body(r), 0)[1], 0)

    def over_rows(total, size, body):
        repeat(total // size, lambda r: body(rows_of(r, size)))

    load_x = pltpu.make_async_copy(x_ref.at[0], a, io_sem.at[0])
    load_x.start()
    fetch(0)
    load_again = pltpu.make_async_copy(x_ref.at[0], dgu.at[0], io_sem.at[1])
    load_again.start()
    load_dy = pltpu.make_async_copy(dy_ref.at[0], up, io_sem.at[2])
    load_dy.start()
    ssq[...] = jnp.zeros_like(ssq)
    load_x.wait()

    def norm_in_place(rows):
        wide = a[rows, :].astype(F32)
        a[rows, :] = (wide * inverse_size(wide)).astype(BF16)

    over_rows(T, RD, norm_in_place)

    def forward(j):
        slot = j % 2
        fetched(j)
        fetch(j + 1)

        def tile(rows):
            gu = dot(a[rows, :], wgu[slot])
            gate, lift = gu[:, :FS], gu[:, FS:]
            hidden = (gate * jax.nn.sigmoid(gate) * lift).astype(BF16)
            acc[rows, :] = jnp.where(j > 0, acc[rows, :], 0.0) + dot(hidden, wd[slot])

        over_rows(T, RF, tile)

    repeat(PARTS, forward)

    load_again.wait()
    load_dy.wait()

    def close_forward(rows):
        h = dgu[0, rows, :].astype(F32) + acc[rows, :].astype(BF16).astype(F32)
        h = h.astype(BF16)
        dgu[0, rows, :] = h
        wide = h.astype(F32)
        normed = (wide * inverse_size(wide)).astype(BF16)
        a[rows, :] = normed
        at[:, rows] = normed.T
        upt[:, rows] = up[rows, :].T

    over_rows(T, RD, close_forward)
    save_h = pltpu.make_async_copy(dgu.at[0], h_ref, io_sem.at[0])
    save_h.start()
    pl.semaphore_wait(barrier, 2 * CHIPS - 1)
    save_h.wait()

    reload_x = pltpu.make_async_copy(x_ref.at[0], a, io_sem.at[1])
    load_h = pltpu.make_async_copy(h_ref, dgu.at[0], io_sem.at[0])

    def cross_layers():
        reload_x.wait()
        load_h.wait()

        def tile(rows):
            wide = a[rows, :].astype(F32)
            normed = (wide * inverse_size(wide)).astype(BF16)
            a[rows, :] = normed
            at[:, rows] = normed.T
            wide = dgu[0, rows, :].astype(F32)
            scale = inverse_size(wide)
            da = acc[rows, :].astype(BF16).astype(F32)
            along = jnp.sum(da * wide, -1, keepdims=True) * (1.0 / D)
            dh = (scale * da - wide * (scale * scale * scale * along)).astype(BF16)
            new = (up[rows, :].astype(F32) + dh.astype(F32)).astype(BF16)
            up[rows, :] = new
            upt[:, rows] = new.T

        over_rows(T, RD, tile)

    def half_of(core):
        return pl.ds(pl.multiple_of(core * half, half), half)

    def pair_copy(n):
        i, p = n // 3, n % 3
        return pltpu.make_async_remote_copy(
            src_ref=gb.at[i % 2, p, half_of(1 - c), :], dst_ref=pair_ref.at[i, p], send_sem=pair_send.at[i % 2, p], recv_sem=pair_recv.at[i, p],
            device_id={"dp": mate}, device_id_type=MESH,
        )

    def own_copy(n):
        i, p = n // 3, n % 3
        return pltpu.make_async_copy(gb.at[i % 2, p, half_of(c), :], own_ref.at[i, p], own_sem.at[i % 2, p])

    class Way:
        def __init__(self, d):
            self.d = d
            self.place = z if d == 0 else last - z
            self.step = 2 if d == 0 else -2
            self.small = pl.ds(d * quarter, quarter)
            self.block = 2 * d + c

        def loads(self, n):
            d, i, p = self.d, n // 3, n % 3
            return (
                pltpu.make_async_copy(own_ref.at[i, p, self.small, :], st.at[d, 0], ld_sem.at[d, 0]),
                pltpu.make_async_copy(pair_ref.at[i, p, self.small, :], st.at[d, 1], ld_sem.at[d, 1]),
                pltpu.make_async_copy(chain_ref.at[d, i, p], st.at[d, 2], ld_sem.at[d, 2]),
            )

        def hop(self, n):
            d, i, p = self.d, n // 3, n % 3
            return pltpu.make_async_remote_copy(
                src_ref=out.at[d, n % SLOTS], dst_ref=chain_ref.at[d, i, p], send_sem=chain_send.at[d, n % SLOTS], recv_sem=chain_recv.at[d, i, p],
                device_id={"dp": (dp + self.step) % (2 * CHIPS)}, device_id_type=MESH,
            )

        def keep(self, n):
            return pltpu.make_async_copy(out.at[self.d, n % SLOTS], g_ref.at[n // 3, n % 3, self.block], keep_sem.at[n % SLOTS])

        def spread(self, n):
            d, i, p = self.d, n // 3, n % 3
            return pltpu.make_async_remote_copy(
                src_ref=g_ref.at[i, p, self.block], dst_ref=g_ref.at[i, p, self.block], send_sem=pass_send.at[d, i, p], recv_sem=pass_recv.at[d, i, p],
                device_id={"dp": (dp - self.step + 2 * CHIPS) % (2 * CHIPS)}, device_id_type=MESH,
            )

        def share(self, n):
            d, i, p = self.d, n // 3, n % 3
            return pltpu.make_async_remote_copy(
                src_ref=g_ref.at[i, p, self.block], dst_ref=g_ref.at[i, p, self.block], send_sem=mate_send.at[d, i, p], recv_sem=mate_recv.at[d, i, p],
                device_id={"dp": mate}, device_id_type=MESH,
            )

        def reaches(self, n, place):
            return (n // 3 < WHOLE) | ((n // 3 == WHOLE) & (place >= last - 1))

        def holds(self, n):
            return (self.place == last) | self.reaches(n, self.place)

        def passes(self, n):
            return (self.place > 0) & self.reaches(n, self.place - 1)

    ways = (Way(0), Way(1))

    def inside(n):
        return (n >= 0) & (n < UNITS)

    def unit(k):
        return jnp.where(k < 3 * PARTS, k, jnp.where(k < 3 * PARTS + PARTS, -1, k - PARTS))

    def start_tick(k):
        newest = unit(k - 2)

        @pl.when(inside(newest))
        def _():
            own_copy(newest).wait()
            pair_copy(newest).wait_recv()

        for way in ways:
            n = unit(k - 2 - LAG * way.place)

            @pl.when(inside(n))
            def _(way=way, n=n):
                own, pair, chain = way.loads(n)
                own.start()
                pair.start()

                @pl.when(way.place > 0)
                def _():
                    way.hop(n).wait_recv()
                    chain.start()

    def finish_tick(k):
        for way in ways:
            d = way.d
            n = unit(k - 2 - LAG * way.place)

            @pl.when(inside(n))
            def _(way=way, d=d, n=n):
                own, pair, chain = way.loads(n)
                own.wait()
                pair.wait()

                @pl.when((way.place < last) & (n >= SLOTS))
                def _():
                    way.hop(n - SLOTS).wait_send()

                def add(so_far):
                    wide = st[d, 0].astype(F32) + st[d, 1].astype(F32)
                    if so_far:
                        wide += st[d, 2].astype(F32)
                    rounded = wide.astype(BF16)
                    out[d, n % SLOTS] = rounded
                    return rounded.astype(F32)

                @pl.when(way.place == 0)
                def _():
                    add(False)
                    way.hop(n).start()

                @pl.when((way.place > 0) & (way.place < last))
                def _():
                    chain.wait()
                    add(True)
                    way.hop(n).start()

                @pl.when(way.place == last)
                def _():
                    chain.wait()
                    total = add(True)
                    way.keep(n).start()
                    ssq[...] += jnp.sum((total * total).reshape(quarter // 8, 8, FS), 0)

        for way in ways:
            n = unit(k - 3 - LAG * (2 * last - way.place))

            @pl.when(inside(n))
            def _(way=way, n=n):
                @pl.when(way.place == last)
                def _():
                    way.keep(n).wait()

                @pl.when((way.place < last) & way.holds(n))
                def _():
                    way.spread(n).wait_recv()

                @pl.when(way.passes(n))
                def _():
                    way.spread(n).start()

                @pl.when(way.holds(n))
                def _():
                    way.share(n).start()

    def dgu_copy(t):
        return pltpu.make_async_copy(dgu.at[t % 2], dgu_ref.at[t], dgu_sem.at[t % 2])

    def backward(t, tick, w, early):
        slot, half_slot = w % 2, t % 2
        fetched(w)

        @pl.when(w < 4 * PARTS - 1)
        def _():
            fetch(w + 1)

        if early:

            @pl.when((t >= 2) & (t < PARTS))
            def _():
                dgu_copy(t - 2).wait()

        def hidden_half(k):
            start_tick(tick + k)

            def tile(r):
                rows = rows_of(k * (T // RT // 2) + r, RT)
                gu = dot(a[rows, :], wgu[slot])
                dh = dot_nt(up[rows, :], wd[slot]).astype(BF16).astype(F32)
                gate, lift = gu[:, :FS], gu[:, FS:]
                s = jax.nn.sigmoid(gate)
                silu = gate * s
                hid[rows, :] = (silu * lift).astype(BF16)
                dgu[half_slot, rows, :FS] = (dh * lift * (s + silu * (1.0 - s))).astype(BF16)
                dgu[half_slot, rows, FS:] = (dh * silu).astype(BF16)

            repeat(T // RT // 2, tile)
            finish_tick(tick + k)

        repeat(2, hidden_half)

        if early:

            @pl.when(t < KEPT)
            def _():
                dgu_copy(t).start()

        @pl.when(t >= 2)
        def _():
            for p in range(3):
                pair_copy(3 * (t - 2) + p).wait_send()

        def down_half(k):
            rows = half_of(jnp.where(k == 0, 1 - c, c))
            gb[half_slot, 0, rows, :] = dot(upt[rows, :], hid[...]).astype(BF16)

            @pl.when(k == 0)
            def _():
                pair_copy(3 * t).start()

            @pl.when(k == 1)
            def _():
                own_copy(3 * t).start()

        repeat(2, down_half)

        def both_half(k):
            @pl.when(k == 1)
            def _():
                start_tick(tick + 2)

            rows = half_of(jnp.where(k == 0, 1 - c, c))
            both = dot(at[rows, :], dgu[half_slot]).astype(BF16)
            gb[half_slot, 1, rows, :] = both[:, :FS]
            gb[half_slot, 2, rows, :] = both[:, FS:]

            @pl.when(k == 0)
            def _():
                pair_copy(3 * t + 1).start()
                pair_copy(3 * t + 2).start()

            @pl.when(k == 1)
            def _():
                own_copy(3 * t + 1).start()
                own_copy(3 * t + 2).start()
                finish_tick(tick + 2)

        repeat(2, both_half)

    def dgu_load(s):
        return pltpu.make_async_copy(dgu_ref.at[s + KEPT - PARTS], dgu.at[s % 2], dgu_sem.at[s % 2])

    def sum_for_a(s):
        w = 2 * PARTS + s
        fetched(w)
        fetch(w + 1)

        @pl.when(s >= PARTS - KEPT)
        def _():
            dgu_load(s).wait()

        @pl.when((s >= 1) & (s < PARTS - 1))
        def _():
            dgu_load(s + 1).start()

        @pl.when(s == PARTS - 1)
        def _():
            load_h.start()

        start_tick(3 * PARTS + s)

        def tile(rows):
            acc[rows, :] = jnp.where(s > 0, acc[rows, :], 0.0) + dot_nt(dgu[s % 2, rows, :], wgu[w % 2])

        over_rows(T, RT, tile)
        finish_tick(3 * PARTS + s)

    def slice_of(i):
        @pl.when(i == PARTS)
        def _():
            reload_x.start()
            repeat(PARTS, sum_for_a)
            cross_layers()

        later = i >= PARTS
        backward(i, jnp.where(later, 3 * i + PARTS, 3 * i), jnp.where(later, i + 2 * PARTS, i + PARTS), True)

    repeat(NS, slice_of)

    def drain(k):
        start_tick(UNITS + PARTS + k)
        finish_tick(UNITS + PARTS + k)

    ticks = max(UNITS + 2 + LAG * last + 1, 3 * (WHOLE + last - 1) + 2 + LAG * 2 * last + 1)
    repeat(ticks - UNITS, drain)

    folded[...] = sum(ssq[:, k * FOLD : (k + 1) * FOLD] for k in range(FS // FOLD))

    def squares(k, slot):
        return pltpu.make_async_remote_copy(
            src_ref=folded, dst_ref=ssq_ref.at[slot], send_sem=ssq_send.at[k], recv_sem=ssq_recv.at[slot],
            device_id={"dp": (dp + k) % (2 * CHIPS)}, device_id_type=MESH,
        )

    def holder(slot):
        return 2 * last * (slot // 2) + slot % 2

    for slot in range(4):

        @pl.when(dp == holder(slot))
        def _(slot=slot):
            pltpu.make_async_copy(folded, ssq_ref.at[slot], io_sem.at[0]).start()
            for k in range(1, 2 * CHIPS):
                squares(k, slot).start()

    for p in range(3):
        pair_copy(3 * (NS - 2) + p).wait_send()
        pair_copy(3 * (NS - 1) + p).wait_send()

    for way in ways:

        @pl.when(way.place < last)
        def _(way=way):
            repeat(SLOTS, lambda k: way.hop(UNITS - SLOTS + k).wait_send())

        def close(n, way=way):
            @pl.when(way.passes(n))
            def _():
                way.spread(n).wait_send()

            @pl.when(way.holds(n))
            def _():
                way.share(n).wait()

        repeat(UNITS, close)

    first = WHOLE + jnp.where(c == 0, z, last - z) - 2
    loads, stores = [], []
    for p in range(3):
        for core in range(2):
            staged = wgu.at[p % 2, pl.ds(p // 2 * half + core * quarter, quarter), pl.ds(0, FS)]
            loads.append(pltpu.make_async_copy(g_ref.at[first, p, 2 * c + core], staged, w_sem.at[core, p]))
            stores.append(pltpu.make_async_copy(staged, sent_ref.at[0, p, core], w_sem.at[core, p]))
    for load in loads:
        load.start()
    for load, store in zip(loads, stores, strict=True):
        load.wait()
        store.start()
    for store in stores:
        store.wait()

    for slot in range(4):

        @pl.when(dp == holder(slot))
        def _(slot=slot):
            pltpu.make_async_copy(folded, ssq_ref.at[slot], io_sem.at[0]).wait()
            for k in range(1, 2 * CHIPS):
                squares(k, slot).wait_send()

        @pl.when(dp != holder(slot))
        def _(slot=slot):
            squares(0, slot).wait_recv()


def gradients(x, dy, w_gate, w_up, w_down):
    _, T, D = x.shape
    F = w_gate.shape[2]
    FS = F // PARTS
    RF, RT, RD = min(1024, T), min(512, T // 2), min(256, T)
    anywhere = pl.BlockSpec(memory_space=pl.ANY)
    dma = pltpu.SemaphoreType.DMA
    return pl.pallas_call(
        functools.partial(gradients_kernel, (T, D, FS, RF, RT, RD)),
        out_shape=(
            jax.ShapeDtypeStruct((NS, 3, 4, D // 4, FS), BF16),
            jax.ShapeDtypeStruct((NS, 3, D // 2, FS), BF16),
            jax.ShapeDtypeStruct((NS, 3, D // 2, FS), BF16),
            jax.ShapeDtypeStruct((2, NS, 3, D // 4, FS), BF16),
            jax.ShapeDtypeStruct((4, 8, FOLD), F32),
            jax.ShapeDtypeStruct((1, 3, 2, D // 4, FS), BF16),
            jax.ShapeDtypeStruct((T, D), BF16),
            jax.ShapeDtypeStruct((KEPT, T, 2 * FS), BF16),
        ),
        in_specs=[anywhere] * 5,
        out_specs=(anywhere,) * 8,
        scratch_shapes=[
            pltpu.VMEM((T, D), BF16),
            pltpu.VMEM((D, T), BF16),
            pltpu.VMEM((T, D), BF16),
            pltpu.VMEM((D, T), BF16),
            pltpu.VMEM((T, D), F32),
            pltpu.VMEM((2, D, 2 * FS), BF16),
            pltpu.VMEM((2, FS, D), BF16),
            pltpu.VMEM((T, FS), BF16),
            pltpu.VMEM((2, T, 2 * FS), BF16),
            pltpu.VMEM((2, 3, D, FS), BF16),
            pltpu.VMEM((2, 3, D // 4, FS), BF16),
            pltpu.VMEM((2, SLOTS, D // 4, FS), BF16),
            pltpu.VMEM((8, FS), F32),
            pltpu.VMEM((8, FOLD), F32),
            dma((2, 3)),
            dma((3,)),
            dma((2,)),
            dma((2, 3)),
            dma((2, 3)),
            dma((NS, 3)),
            dma((2, 3)),
            dma((2, SLOTS)),
            dma((2, NS, 3)),
            dma((SLOTS,)),
            dma((2, WHOLE + CHIPS, 3)),
            dma((2, WHOLE + CHIPS, 3)),
            dma((2, NS, 3)),
            dma((2, NS, 3)),
            dma((2 * CHIPS,)),
            dma((4,)),
        ],
        compiler_params=pltpu.CompilerParams(collective_id=0, has_side_effects=True, vmem_limit_bytes=66_000_000),
        name="gradients",
    )(x, dy, w_gate, w_up, w_down)


SUBS, DEEP = 4, 6


def adamw_kernel(count, work, n_in, aliased, *refs):
    refs = list(refs)

    def take(n):
        out, refs[:n] = refs[:n], []
        return out

    ssq_ref, g_ref = take(2)
    back = take(n_in)
    arrays = take(9)
    take(9 if aliased else 0)
    results = take(9)
    bufs, outs = take(9), take(9)
    gv, squares, g_sem, in_sem, out_sem, squares_sem = take(6)
    quarter, FS = gv.shape[2:]
    few, part = quarter // SUBS, FS // SUBS
    dp = lax.axis_index("dp")
    z, c = dp // 2, dp % 2
    total = SUBS * len(work)
    numbers = [4 * i + b for i, b, _ in work]
    cut = next((k for k in range(1, len(work)) if numbers[k] != numbers[k - 1] + 1), len(work))

    def here(k, source):
        return pltpu.make_async_copy(source, gv.at[k], g_sem.at[k])

    def fetch(k):
        i, b, came = work[k]
        place = z if b < 2 else CHIPS - 1 - z
        for p in range(CHIPS):
            if came[p] is None:

                @pl.when(place == p)
                def _():
                    here(k, g_ref.at[i, :, b]).start()

            else:
                for core in range(2):

                    @pl.when((place == p) & (c == core))
                    def _(at=came[p][0 if core == b // 2 else 1]):
                        here(k, back[at].at[0, :, b % 2]).start()

    def blocks(n):
        k, sub = n // SUBS, n % SUBS
        at = numbers[0] + k if cut == len(work) else jnp.where(k < cut, numbers[0] + k, numbers[cut] - cut + k)
        i, b = at // 4, at % 4
        layer, hidden, q = 1 - i // PARTS, i % PARTS, b % 2 * 2 + b // 2
        across = (layer, pl.ds(pl.multiple_of(q * quarter + sub * few, few), few), pl.ds(pl.multiple_of(hidden * FS, FS), FS))
        down = (layer, pl.ds(pl.multiple_of(hidden * FS + sub * part, part), part), pl.ds(pl.multiple_of(q * quarter, quarter), quarter))
        return across, across, down

    def copies(n, inward):
        slot, where = n % DEEP, blocks(n)
        if inward:
            return [pltpu.make_async_copy(arrays[k].at[where[k % 3]], bufs[k].at[slot], in_sem.at[slot]) for k in range(9)]
        return [pltpu.make_async_copy(outs[k].at[slot], results[k].at[where[k % 3]], out_sem.at[slot]) for k in range(9)]

    def start(n, inward):
        for copy in copies(n, inward):
            copy.start()

    def wait(n, inward):
        for copy in copies(n, inward):
            copy.wait()

    load_squares = pltpu.make_async_copy(ssq_ref, squares, squares_sem)
    load_squares.start()
    fetch(0)
    for n in range(min(DEEP - 1, total)):
        start(n, True)
    for k in range(1, len(work)):
        fetch(k)
    load_squares.wait()
    factor = jnp.minimum(1.0, 0.5 * lax.rsqrt(jnp.sum(squares[...]) / count + 1e-30))

    def piece(n, _):
        k, sub, slot = n // SUBS, n % SUBS, n % DEEP

        @pl.when(sub == 0)
        def _():
            here(k, g_ref.at[0, :, 0]).wait()

        @pl.when(n + DEEP - 1 < total)
        def _():
            start(n + DEEP - 1, True)

        wait(n, True)

        @pl.when(n >= DEEP)
        def _():
            wait(n - DEEP, False)

        def update(number, g):
            g = g * factor
            m = 0.9 * bufs[3 + number][slot] + 0.1 * g
            v = 0.95 * bufs[6 + number][slot] + 0.05 * g * g
            w = bufs[number][slot].astype(F32)
            outs[number][slot] = (w - 0.02 * (m * lax.rsqrt(v + 1e-8) + 0.1 * w)).astype(BF16)
            outs[3 + number][slot] = m
            outs[6 + number][slot] = v

        rows = pl.ds(pl.multiple_of(sub * few, few), few)
        update(0, gv[k, 1, rows, :].astype(F32))
        update(1, gv[k, 2, rows, :].astype(F32))
        update(2, gv[k, 0, :, pl.ds(pl.multiple_of(sub * part, part), part)].astype(F32).T)
        start(n, False)
        return 0

    lax.fori_loop(0, total, piece, 0)
    lax.fori_loop(max(total - DEEP, 0), total, lambda n, _: (wait(n, False), 0)[1], 0)


def adamw(ssq, g, arrays, results, listed, back):
    _, _, _, quarter, FS = g.shape
    anywhere = pl.BlockSpec(memory_space=pl.ANY)
    size = 3 * len(listed) * quarter * FS
    ins = [ssq, g, *back, *arrays, *(results or ())]
    shapes = [(DEEP, quarter // SUBS, FS)] * 2 + [(DEEP, FS // SUBS, quarter)]
    bufs = [pltpu.VMEM(shapes[k % 3], a.dtype) for k, a in enumerate(arrays)]
    return pl.pallas_call(
        functools.partial(adamw_kernel, float(g.size), listed, len(back), bool(results)),
        in_specs=[anywhere] * len(ins),
        out_specs=[anywhere] * 9,
        out_shape=[jax.ShapeDtypeStruct(a.shape, a.dtype) for a in arrays],
        input_output_aliases={len(ins) - 9 + k: k for k in range(9)} if results else {},
        scratch_shapes=[
            *bufs,
            *bufs,
            pltpu.VMEM((len(listed), 3, quarter, FS), BF16),
            pltpu.VMEM(ssq.shape, F32),
            pltpu.SemaphoreType.DMA((len(listed),)),
            pltpu.SemaphoreType.DMA((DEEP,)),
            pltpu.SemaphoreType.DMA((DEEP,)),
            pltpu.SemaphoreType.DMA,
        ],
        compiler_params=pltpu.CompilerParams(vmem_limit_bytes=66_000_000),
        cost_estimate=pl.CostEstimate(flops=16 * size, bytes_accessed=22 * size, transcendentals=size),
        name="adamw",
    )(*ins)


def load_kernel(i, g_ref, _, sent_ref, buf, sem):
    dp = lax.axis_index("dp")
    z, c = dp // 2, dp % 2

    @pl.when(z == (CHIPS - 1) * (1 - c))
    def _():
        pieces = buf.shape[0]
        loads = [pltpu.make_async_copy(g_ref.at[i, p, pl.ds(2 * c, 2)], buf.at[p], sem.at[0, p]) for p in range(pieces)]
        stores = [pltpu.make_async_copy(buf.at[p], sent_ref.at[0, p], sem.at[1, p]) for p in range(pieces)]
        for load in loads:
            load.start()
        for load, store in zip(loads, stores, strict=True):
            load.wait()
            store.start()
        for store in stores:
            store.wait()


def load(g, i, came):
    anywhere = pl.BlockSpec(memory_space=pl.ANY)
    return pl.pallas_call(
        functools.partial(load_kernel, i),
        in_specs=[anywhere, anywhere],
        out_specs=anywhere,
        out_shape=jax.ShapeDtypeStruct(came.shape, came.dtype),
        input_output_aliases={1: 0},
        scratch_shapes=[pltpu.VMEM(came.shape[1:], BF16), pltpu.SemaphoreType.DMA((2, 3))],
        compiler_params=pltpu.CompilerParams(vmem_limit_bytes=66_000_000),
        cost_estimate=pl.CostEstimate(flops=came.size, bytes_accessed=4 * came.size, transcendentals=0),
        name="load",
    )(g, came)


def finish(g, ssq, sent, arrays):
    last = CHIPS - 1
    units_left = NS - WHOLE
    stages = units_left + 1
    ready = [(i, b, (None,) * CHIPS) for i in range(WHOLE) for b in range(4)]
    first = min(6, 2 * WHOLE)
    spare = 4 * WHOLE - 3 * first
    more = [spare // (stages - 3) + (s < spare % (stages - 3)) for s in range(stages - 3)] + [0] * 2
    back, index, results = [], {}, None

    def units(u):
        came = tuple(index[u - p + 1] if p < last and u - p + 1 >= 0 else None for p in range(CHIPS))
        return [(WHOLE + u, b, came) for b in range(4)]

    def update(results, listed):
        used = sorted({at for _, _, came in listed for pair in came if pair for at in pair})
        where = {at: k for k, at in enumerate(used)}
        listed = [(i, b, tuple(pair and tuple(where[at] for at in pair) for pair in came)) for i, b, came in listed]
        return adamw(ssq, g, arrays, results, listed, [back[at] for at in used])

    def device(place, core):
        return 2 * (place if core == 0 else last - place) + core

    pending = None
    for s in range(stages + 2):
        if s < stages:
            moves = [(device(p, core), device(p - 1, core)) for p in range(1, CHIPS) if 0 <= s + p - 2 < units_left for core in range(2)]
            newest = lax.ppermute(sent, "dp", moves)
        if pending is not None:
            back.append(lax.ppermute(*pending))
            pending = None
        many = first if s < 3 else more[s - 3]
        listed, ready = ready[:many], ready[many:]
        if s >= 3:
            listed = listed + units(s - 3)
        results = update(results, listed)
        if s < stages:
            sent = load(g, WHOLE + s + last - 1, newest) if s + last - 1 < units_left else newest
            index[s] = (len(back), len(back) + 1)
            back.append(sent)
            pending = (sent, "dp", [(to, to + 1 - 2 * (to % 2)) for _, to in moves])
    return results


def solution(mesh):
    def step(x, dy, *arrays):
        g, *_, ssq, sent, _, _ = gradients(x, dy, *arrays[:3])
        return tuple(finish(g, ssq, sent, arrays))

    return jax.shard_map(
        step,
        mesh=mesh,
        in_specs=(P(("rep", "dp"), None, None),) * 2 + (P(None, None, None),) * 9,
        out_specs=(P("rep", None, None),) * 9,
        check_vma=False,
    )
```
